512 devices in a mesh: agent: 16 (over x, z_lo, core), tp: 32 (over z_hi, y).
Axes of the slice: x: 4, y: 8, z: 8 (z_hi: 4, z_lo: 2; z = z_hi * 2 + z_lo), core: 2. Of those that a mesh axis runs over, the one named last changes fastest.
Arguments:
- tokens: bfloat16 [16, 512, 2048], P('agent', 'tp'), may hold values from -6 to 6
- targets: bfloat16 [16, 512, 2048], P('agent', 'tp'), may hold values from -6 to 6
- params: bfloat16 [16, 2048, 8192], P('agent', None, 'tp'), may hold values from -6 to 6
- tracker: bfloat16 [16, 2048, 8192], P('agent', None, 'tp'), may hold values from -6 to 6
- up_weight: bfloat16 [2048, 8192], P('agent', 'tp'), may hold values from -0.125 to 0.125
- down_weight: bfloat16 [8192, 2048], P('tp', 'agent'), may hold values from -0.0625 to 0.0625
- edge_weight: float32 [16], replicated, may hold values from 0.1 to 0.4
- step_size: float32 [1], replicated, may hold values from 0.1 to 0.5
Outputs:
- new_params: bfloat16 [16, 2048, 8192], P('agent', None, 'tp')
- new_tracker: bfloat16 [16, 2048, 8192], P('agent', None, 'tp')
The draws below stay inside these ranges and needn't reach their ends.
All inputs are finite; a program needn't handle non-finite values.
Results may differ from the reference program's by a relative error of at most 0.033.
Values may be sent and summed in bfloat16 or wider, within the bound.
A program may use at most 64 MiB of HBM per device.

```python
import math
import jax
import jax.numpy as jnp
from jax import lax

D = 2048
FF = 8192
TOKENS = 512
AGENTS = 16
N_TP = 32


def shard_levels(key, dims, cuts, least, top_value):
    def one(position, parts):
        heights = jax.random.uniform(jax.random.fold_in(jax.random.fold_in(key, 6), position), (parts,), jnp.float32, least / len(cuts), top_value / len(cuts))
        return jnp.repeat(jnp.exp(heights), dims[position] // parts).reshape((-1,) + (1,) * (len(dims) - position - 1))

    factor_of = one(*cuts[0])
    for cut in cuts[1:]:
        factor_of = factor_of * one(*cut)
    return factor_of


def normal_values(rng, shape, deviation, bound, cuts=(), dtype=jnp.bfloat16):
    entries = deviation * jax.random.normal(rng, shape, jnp.float32)
    if cuts:
        entries = entries * shard_levels(rng, shape, cuts, -0.22, 0.18)
    return jnp.clip(entries, -bound, bound).astype(dtype)


def setup_inputs(seed: int = 0) -> dict:
    keys = jax.random.split(jax.random.key(seed), 9)
    return {
        "tokens": normal_values(keys[0], (AGENTS, TOKENS, D), 1.0, 6.0, ((0, 16), (1, 32))),
        "targets": normal_values(keys[1], (AGENTS, TOKENS, D), 1.0, 6.0, ((0, 16), (1, 32))),
        "params": normal_values(keys[2], (AGENTS, D, FF), 1.0, 6.0, ((0, 16), (2, 32))),
        "tracker": normal_values(keys[3], (AGENTS, D, FF), 1.0, 6.0, ((0, 16), (2, 32))),
        "up_weight": normal_values(keys[4], (D, FF), D ** -0.5, 0.125, ((0, 16), (1, 32))),
        "down_weight": normal_values(keys[5], (FF, D), FF ** -0.5, 0.0625, ((0, 32), (1, 16))),
        "edge_weight": jnp.clip(jax.random.uniform(keys[6], (AGENTS,), jnp.float32, 0.1, 0.4), 0.1, 0.4),
        "step_size": jnp.clip(jnp.exp(jax.random.uniform(keys[7], (1,), jnp.float32, math.log(0.1), math.log(0.5))), 0.1, 0.5),
    }


def gate_grad(tok, param, up_weight, down_weight, target):
    scale = 1.0 / D ** 0.5
    gate = jnp.dot(tok, param, preferred_element_type=jnp.float32) * scale
    up = jnp.dot(tok, up_weight, preferred_element_type=jnp.float32)
    hidden = (jax.nn.sigmoid(gate) * gate * up).astype(jnp.bfloat16)
    group = FF // N_TP
    hidden_groups = hidden.reshape(hidden.shape[0], N_TP, group).transpose(1, 0, 2)
    down_groups = down_weight.reshape(N_TP, group, down_weight.shape[1])

    def add_share(total, items):
        piece, weights = items
        share = jnp.dot(piece, weights, preferred_element_type=jnp.float32).astype(jnp.bfloat16)
        return (total + share.astype(jnp.float32), None)
    start = jnp.zeros((hidden.shape[0], down_weight.shape[1]), jnp.float32)
    out, unused = lax.scan(add_share, start, (hidden_groups, down_groups))
    err = (2.0 * (out - target.astype(jnp.float32))).astype(jnp.bfloat16)
    back = jnp.dot(err, down_weight.T, preferred_element_type=jnp.float32)
    sig = jax.nn.sigmoid(gate)
    dgate = (back * up * sig * (1.0 + gate * (1.0 - sig))).astype(jnp.bfloat16)
    return jnp.dot(tok.T, dgate, preferred_element_type=jnp.float32) * scale

def reference(tokens, targets, params, tracker, up_weight, down_weight, edge_weight, step_size):
    params32 = params.astype(jnp.float32)
    tracker32 = tracker.astype(jnp.float32)
    e_right = edge_weight
    e_left = jnp.roll(edge_weight, 1)
    own = 1.0 - e_right - e_left
    e_right = e_right[:, None, None]
    e_left = e_left[:, None, None]
    own = own[:, None, None]
    mixed_x = own * params32 + e_right * jnp.roll(params32, -1, axis=0) + e_left * jnp.roll(params32, 1, axis=0)
    mixed_y = own * tracker32 + e_right * jnp.roll(tracker32, -1, axis=0) + e_left * jnp.roll(tracker32, 1, axis=0)
    new_params = (mixed_x - step_size[0] * tracker32).astype(jnp.bfloat16)

    def one_agent(items):
        tok, target, param, fresh = items
        before = gate_grad(tok, param, up_weight, down_weight, target)
        after = gate_grad(tok, fresh, up_weight, down_weight, target)
        return after - before
    change = lax.map(one_agent, (tokens, targets, params, new_params))
    new_tracker = (mixed_y + change).astype(jnp.bfloat16)
    return (new_params, new_tracker)
```

```python
import functools

import jax
import jax.numpy as jnp
from jax import lax
from jax.experimental import pallas as pl
from jax.experimental.pallas import tpu as pltpu
from jax.sharding import PartitionSpec as P

MESH = pl.DeviceIdType.MESH
BF16 = jnp.bfloat16
F32 = jnp.float32
ORDER = (0, 7, 1, 6, 2, 5, 3, 4)
TRACK_PIECES = 4


class Plan:
    def __init__(self):
        self.count = 0

    def take(self, *shape):
        size = 1
        for n in shape:
            size *= n
        base = self.count
        self.count += size

        def number(*index):
            flat = 0
            for i, n in zip(index, shape):
                flat = flat * n + i
            return base + flat

        return number


plan = Plan()
TZ = plan.take(4)
TY = plan.take(2, 5, 4)
UZ, UX, UF, UC = plan.take(1), plan.take(2), plan.take(2), plan.take(1)
DZ, DY = plan.take(1), plan.take(2, 5)
DX, DF, DC = plan.take(2, 8), plan.take(2, 8), plan.take(8)
PI, PO, TI, TO = plan.take(1), plan.take(1), plan.take(1), plan.take(TRACK_PIECES)
HI, RS, EG, BK = plan.take(2, 8), plan.take(2, 4), plan.take(2, 4), plan.take(2, 8)
SEMS = plan.count


def kernel(
    edge, step, tokens, targets, params, tracker, up_w, down_w, fresh_out, track_out,
    tok, tgt, pbuf, tbuf, pin, pof, tin, tof, fresh, upb, dwn, upv, fac, hsend, hall,
    psend, prec, eall, bsend, brec, dd, trk, ssem, rsem, lsem,
):
    a = lax.axis_index("agent")
    t = lax.axis_index("tp")
    x, zl, c = a // 4, (a // 2) % 2, a % 2
    zh, y = t // 8, t % 8
    scale = 2048.0 ** -0.5

    def along_y(r):
        return (a, zh * 8 + (y + r) % 8)

    def along_z(q):
        return (a, ((zh + q) % 4) * 8 + y)

    def along_x(r):
        return ((a + 4 * r + 16) % 16, t)

    other_core = (a + 1 - 2 * c, t)
    off_chip = ((a + 2 * c + 15) % 16, t)
    other_z = (a + 2 - 4 * zl, t)

    def cols(first, n):
        return pl.ds(first, n)

    local = []

    def fetch(src, dst):
        copy = pltpu.make_async_copy(src, dst, lsem.at[len(local)])
        copy.start()
        local.append(copy)
        return copy

    up_own = upb.at[x, zl, c]
    got_tok = fetch(tokens.at[0], tok.at[cols(0, 16)])
    got_up = fetch(up_w, up_own)
    got_down = fetch(down_w, dwn.at[cols(0, 256), cols(0, 128)])
    got_p = fetch(params.at[0], pbuf)
    got_t = fetch(tracker.at[0], tbuf)
    got_tgt = []
    for rc in range(2):
        for rx in range(4):
            for rz in range(2):
                who = ((x + rx) % 4) * 4 + ((zl + rz) % 2) * 2 + (c + rc) % 2
                src = targets.at[0, :, pl.ds(pl.multiple_of(who * 128, 128), 128)]
                got_tgt.append(fetch(src, tgt.at[:, cols(rc * 1024 + rx * 256 + rz * 128, 128)]))

    barrier = pltpu.get_barrier_semaphore()
    peers = [other_core, off_chip, other_z, along_x(1), along_x(-1)]
    peers += [along_y(r) for r in range(1, 8)] + [along_z(q) for q in range(1, 4)]
    for peer in peers:
        pl.semaphore_signal(barrier, inc=1, device_id=peer, device_id_type=MESH)
    pl.semaphore_wait(barrier, len(peers))

    sent = []

    def message(src, dst, peer, k):
        return pltpu.make_async_remote_copy(
            src_ref=src, dst_ref=dst, send_sem=ssem.at[k], recv_sem=rsem.at[k],
            device_id=peer, device_id_type=MESH,
        )

    def send(src, dst, peer, k):
        copy = message(src, dst, peer, k)
        copy.start()
        sent.append(copy)

    def arrive(dst, k):
        message(dst, dst, other_core, k).wait_recv()

    def tok_at(r, q):
        return tok.at[cols((r % 8) * 64 + (q % 4) * 16, 16)]

    def dwn_at(r, rx, first=0, rows=256):
        return dwn.at[cols((r % 8) * 256 + first, rows), cols(rx * 256, 256)]

    def tok_steps(way, q):
        return 4 if (q < 2) == (way == 0) else 3

    def tok_step(way, s, q):
        sign = 1 if way == 0 else -1
        send(tok_at(-sign * (s - 1), q), tok_at(-sign * s, q), along_y(sign), TY(way, s, q))

    def tok_wait(way, s, q):
        sign = 1 if way == 0 else -1
        arrive(tok_at(-sign * s, q), TY(way, s, q))

    def dwn_half(way, s):
        return (0, 256) if s < 4 else (128 * way, 128)

    def dwn_step(way, s):
        sign = 1 if way == 0 else -1
        half = dwn_half(way, s)
        send(
            dwn_at(-sign * (s - 1), 0, *half), dwn_at(-sign * s, 0, *half),
            along_y(sign), DY(way, s),
        )

    def dwn_wait(way, s):
        sign = 1 if way == 0 else -1
        arrive(dwn_at(-sign * s, 0, *dwn_half(way, s)), DY(way, s))

    def x_first(r):
        send(dwn_at(r, 0), dwn_at(r, 3), along_x(1), DX(0, r))
        send(dwn_at(r, 0), dwn_at(r, 1), along_x(-1), DX(1, r))

    def x_second(r):
        arrive(dwn_at(r, 3), DX(0, r))
        send(dwn_at(r, 3, 0, 128), dwn_at(r, 2, 0, 128), along_x(1), DF(0, r))
        arrive(dwn_at(r, 1), DX(1, r))
        send(dwn_at(r, 1, 128, 128), dwn_at(r, 2, 128, 128), along_x(-1), DF(1, r))

    def core_half(r, rc):
        return dwn.at[cols((r % 8) * 256, 256), cols(rc * 1024, 1024)]

    def x_third(r):
        arrive(dwn_at(r, 2, 0, 128), DF(0, r))
        arrive(dwn_at(r, 2, 128, 128), DF(1, r))
        send(core_half(r, 0), core_half(r, 1), other_core, DC(r))

    got_tok.wait()
    for d in (1, 3, 2):
        send(tok_at(0, 0), tok_at(0, -d), along_z(d), TZ(d))
    for way in range(2):
        tok_step(way, 1, 0)
    got_up.wait()
    send(up_own, up_own, other_z, UZ(0))
    got_down.wait()
    send(
        dwn.at[cols(0, 256), cols(0, 128)], dwn.at[cols(0, 256), cols(128, 128)], other_z, DZ(0)
    )
    got_p.wait()
    send(pbuf, pof, off_chip, PO(0))
    send(pbuf, pin, other_core, PI(0))
    got_t.wait()
    send(tbuf, tin, other_core, TI(0))
    for copy in got_tgt:
        copy.wait()

    for d in (1, 3, 2):
        arrive(tok_at(0, -d), TZ(d))
        for way in range(2):
            tok_step(way, 1, 4 - d)
    arrive(upb.at[x, 1 - zl, c], UZ(0))
    send(upb.at[x, :, c], upb.at[x, :, c], along_x(1), UX(0))
    send(upb.at[x, :, c], upb.at[x, :, c], along_x(-1), UX(1))
    arrive(dwn.at[cols(0, 256), cols(128, 128)], DZ(0))
    dwn_step(0, 1)
    dwn_step(1, 1)
    x_first(0)

    for s in range(1, 5):
        for q in (0, 3, 1, 2):
            for way in range(2):
                if s <= tok_steps(way, q):
                    tok_wait(way, s, q)
                    if s < tok_steps(way, q):
                        tok_step(way, s + 1, q)
        for way in range(2):
            dwn_wait(way, s)
            if s < 4:
                dwn_step(way, s + 1)
        for r in (8 - s, s)[: 2 if s < 4 else 1]:
            x_first(r)
        if s == 1:
            below, above = (x + 3) % 4, (x + 1) % 4
            arrive(upb.at[below, :, c], UX(0))
            send(upb.at[below, 0, c], upb.at[below, 0, c], along_x(1), UF(0))
            arrive(upb.at[above, :, c], UX(1))
            send(upb.at[above, 1, c], upb.at[above, 1, c], along_x(-1), UF(1))
            x_second(0)
        if s == 2:
            across = (x + 2) % 4
            arrive(upb.at[across, 0, c], UF(0))
            arrive(upb.at[across, 1, c], UF(1))
            send(upb.at[:, :, c], upb.at[:, :, c], other_core, UC(0))
            x_third(0)
            x_second(7)
            x_second(1)
        if s == 3:
            x_third(7)
            x_third(1)
            x_second(6)
            x_second(2)
        if s == 4:
            x_second(5)
            x_second(3)
            x_third(6)
            x_third(2)

    def rows256(i):
        return pl.ds(pl.multiple_of(i * 256, 256), 256)

    arrive(upb.at[:, :, 1 - c], UC(0))

    @pl.loop(0, 2)
    def _(i):
        rows = rows256(i)
        total = jnp.zeros((256, 256), F32)
        for k in range(8):
            total += jnp.dot(
                tok[rows, k * 256 : (k + 1) * 256],
                upb[k // 2, k % 2].reshape(256, 256),
                preferred_element_type=F32,
            )
        upv[rows, :] = total

    def hidden_of(p, weights):
        @pl.loop(0, 2)
        def _(i):
            rows = rows256(i)
            gate = jnp.dot(tok[rows, :], weights[...], preferred_element_type=F32) * scale
            sig = jax.nn.sigmoid(gate)
            up = upv[rows, :]
            hsend[p, rows, :] = (sig * gate * up).astype(BF16)
            fac[p, rows, :] = up * sig * (1.0 + gate * (1.0 - sig))

        for r in (1, 7, 2, 6, 3, 5, 4):
            send(
                hsend.at[p, cols(r * 64, 64)], hall.at[p, :, cols((8 - r) * 256, 256)],
                along_y(r), HI(p, r),
            )
        hall[p, :, 0:256] = hsend[p, 0:64, :]

    hidden_of(0, pbuf)
    x_second(4)

    e_off = edge[(a + c + 15) % 16]
    e_in = edge[(a + 16 - c) % 16]
    own = 1.0 - e_off - e_in
    eta = step[0]
    arrive(pin, PI(0))
    arrive(pof, PO(0))

    def track_piece(k):
        return tof.at[cols(k * (2048 // TRACK_PIECES), 2048 // TRACK_PIECES)]

    def track_send(k):
        rows = cols(k * (2048 // TRACK_PIECES), 2048 // TRACK_PIECES)
        send(tbuf.at[rows], tof.at[rows], off_chip, TO(k))

    track_send(0)
    track_send(1)

    @pl.loop(0, 8)
    def _(i):
        rows = rows256(i)
        mixed = own * pbuf[rows, :].astype(F32)
        mixed += e_off * pof[rows, :].astype(F32) + e_in * pin[rows, :].astype(F32)
        fresh[rows, :] = (mixed - eta * tbuf[rows, :].astype(F32)).astype(BF16)

    fresh_copy = pltpu.make_async_copy(fresh, fresh_out.at[0], lsem.at[len(local)])
    fresh_copy.start()
    hidden_of(1, fresh)
    x_third(5)
    x_third(3)
    x_third(4)
    for r in ORDER:
        arrive(core_half(r, 1), DC(r))

    def partial_of(p):
        for r in range(1, 8):
            arrive(hall.at[p, :, cols((8 - r) * 256, 256)], HI(p, r))

        @pl.loop(0, 8)
        def _(i):
            part = jnp.dot(hall[p], dwn[:, rows256(i)], preferred_element_type=F32)
            psend[p, :, rows256(i)] = part.astype(BF16)

        for q in (1, 3, 2):
            send(psend.at[p, cols(q * 16, 16)], prec.at[p, 4 - q], along_z(q), RS(p, q))

    partial_of(0)
    partial_of(1)

    def err_of(p):
        total = psend[p, 0:16, :].astype(F32)
        for q in (1, 3, 2):
            arrive(prec.at[p, 4 - q], RS(p, q))
            total += prec[p, 4 - q].astype(F32)
        eall[p, 0:16, :] = (2.0 * (total - tgt[...].astype(F32))).astype(BF16)
        for q in (1, 3, 2):
            send(
                eall.at[p, cols(0, 16)], eall.at[p, cols((4 - q) * 16, 16)], along_z(q), EG(p, q)
            )

    err_of(0)
    err_of(1)
    for k in range(2, TRACK_PIECES):
        track_send(k)

    def back_block(p, r):
        return lax.dot_general(
            eall[p], dwn[pl.ds(pl.multiple_of(r * 256, 256), 256), :],
            (((1,), (1,)), ((), ())), preferred_element_type=F32,
        ).astype(BF16)

    def back_message(p, r):
        rows = pl.ds(pl.multiple_of(r * 64, 64), 64)
        land = pl.ds(pl.multiple_of((8 - r) * 64, 64), 64)
        return message(bsend.at[p, rows], brec.at[p, land], along_y(r), BK(p, 0) + r)

    def back_of(p):
        for q in (1, 3, 2):
            arrive(eall.at[p, cols((4 - q) * 16, 16)], EG(p, q))

        @pl.loop(1, 8)
        def _(r):
            bsend[p, pl.ds(pl.multiple_of(r * 64, 64), 64), :] = back_block(p, r)
            back_message(p, r).start()

        brec[p, 0:64, :] = back_block(p, 0)

    back_of(0)
    back_of(1)
    for p in range(2):

        @pl.loop(1, 8)
        def _(r):
            land = pl.ds(pl.multiple_of((8 - r) * 64, 64), 64)
            message(brec.at[p, land], brec.at[p, land], other_core, BK(p, 0) + r).wait_recv()

    dd[...] = (
        brec[1].astype(F32) * fac[1] - brec[0].astype(F32) * fac[0]
    ).astype(BF16)
    arrive(tin, TI(0))
    for k in range(TRACK_PIECES):
        arrive(track_piece(k), TO(k))

    @pl.loop(0, 8)
    def _(i):
        rows = rows256(i)
        change = lax.dot_general(
            tok[:, rows], dd[...], (((0,), (0,)), ((), ())), preferred_element_type=F32
        )
        mixed = own * tbuf[rows, :].astype(F32)
        mixed += e_off * tof[rows, :].astype(F32) + e_in * tin[rows, :].astype(F32)
        trk[rows, :] = (mixed + change * scale).astype(BF16)

    track_copy = pltpu.make_async_copy(trk, track_out.at[0], lsem.at[len(local) + 1])
    track_copy.start()
    for copy in sent:
        copy.wait_send()
    for p in range(2):

        @pl.loop(1, 8)
        def _(r):
            back_message(p, r).wait_send()

    fresh_copy.wait()
    track_copy.wait()


def on_device(tokens, targets, params, tracker, up_weight, down_weight, edge_weight, step_size):
    hbm = pl.BlockSpec(memory_space=pltpu.HBM)
    smem = pl.BlockSpec(memory_space=pltpu.SMEM)
    block = pltpu.VMEM((2048, 256), BF16)
    out = jax.ShapeDtypeStruct(params.shape, BF16)
    return pl.pallas_call(
        kernel,
        out_shape=(out, out),
        in_specs=[smem, smem] + [hbm] * 6,
        out_specs=(hbm, hbm),
        scratch_shapes=[
            pltpu.VMEM((512, 2048), BF16),
            pltpu.VMEM((16, 2048), BF16),
            block, block, block, block, block, block, block,
            pltpu.VMEM((4, 2, 2, 128, 256), BF16),
            pltpu.VMEM((2048, 2048), BF16),
            pltpu.VMEM((512, 256), F32),
            pltpu.VMEM((2, 512, 256), F32),
            pltpu.VMEM((2, 512, 256), BF16),
            pltpu.VMEM((2, 64, 2048), BF16),
            pltpu.VMEM((2, 64, 2048), BF16),
            pltpu.VMEM((2, 4, 16, 2048), BF16),
            pltpu.VMEM((2, 64, 2048), BF16),
            pltpu.VMEM((2, 512, 256), BF16),
            pltpu.VMEM((2, 512, 256), BF16),
            pltpu.VMEM((512, 256), BF16),
            block,
            pltpu.SemaphoreType.DMA((SEMS,)),
            pltpu.SemaphoreType.DMA((SEMS,)),
            pltpu.SemaphoreType.DMA((24,)),
        ],
        compiler_params=pltpu.CompilerParams(
            collective_id=0, has_side_effects=True, vmem_limit_bytes=56 * 1024 * 1024
        ),
    )(edge_weight, step_size, tokens, targets, params, tracker, up_weight, down_weight)


def solution(mesh):
    in_specs = (
        P("agent", "tp", None),
        P("agent", "tp", None),
        P("agent", None, "tp"),
        P("agent", None, "tp"),
        P("agent", "tp"),
        P("tp", "agent"),
        P(),
        P(),
    )
    out_specs = (P("agent", None, "tp"), P("agent", None, "tp"))
    return jax.shard_map(
        on_device, mesh=mesh, in_specs=in_specs, out_specs=out_specs, check_vma=False
    )
```

```python
import functools

import jax
import jax.numpy as jnp
from jax import lax
from jax.experimental import pallas as pl
from jax.experimental.pallas import tpu as pltpu
from jax.sharding import PartitionSpec as P

MESH = pl.DeviceIdType.MESH
BF16 = jnp.bfloat16
F32 = jnp.float32
ORDER = (0, 7, 1, 6, 2, 5, 3, 4)
NEAR = 224
FAR_FIRST = (4, 3, 5, 2, 6, 1, 7)


class Plan:
    def __init__(self):
        self.count = 0

    def take(self, *shape):
        size = 1
        for n in shape:
            size *= n
        base = self.count
        self.count += size

        def number(*index):
            flat = 0
            for i, n in zip(index, shape):
                flat = flat * n + i
            return base + flat

        return number


plan = Plan()
TZ = plan.take(2, 2)
TY = plan.take(2, 5, 4)
UZ, UX, UF, UC = plan.take(1), plan.take(2), plan.take(2), plan.take(1)
DZ, DY, EY = plan.take(1), plan.take(2, 5), plan.take(2, 5)
DX, DF, DC = plan.take(2, 8), plan.take(2, 8), plan.take(8)
D0, DB = plan.take(2), plan.take(2)
PI, PO, TI, TO = plan.take(1), plan.take(3), plan.take(1), plan.take(2)
PR, TR = plan.take(1), plan.take(1)
HI, BK = plan.take(2, 8), plan.take(2, 8)
RS, EG = plan.take(2, 3, 2), plan.take(2, 2, 2)
SEMS = plan.count


def kernel(
    edge, step, tokens, targets, params, tracker, up_w, down_w, fresh_out, track_out,
    tok, tgt, pbuf, tbuf, pin, pof, tin, tof, fresh, upb, dwn, upv, fac, hsend, hall,
    psend, pmid, prec, eall, bsend, brec, dd, trk, prel, trel, turned, mixed_y, ssem, rsem, lsem,
):
    a = lax.axis_index("agent")
    t = lax.axis_index("tp")
    x, zl, c = a // 4, (a // 2) % 2, a % 2
    zh, y = t // 8, t % 8
    scale = 2048.0 ** -0.5

    def along_y(r):
        return (a, zh * 8 + (y + r + 8) % 8)

    def along_z(q):
        return (a, ((zh + q + 4) % 4) * 8 + y)

    def along_x(r):
        return ((a + 4 * r + 16) % 16, t)

    other_core = (a + 1 - 2 * c, t)
    off_chip = ((a + 2 * c + 15) % 16, t)
    other_z = (a + 2 - 4 * zl, t)
    beyond = ((a + 6 * c + 13) % 16, t)
    diagonal = c == zl

    def cols(first, n):
        return pl.ds(first, n)

    local = []

    def fetch(src, dst):
        copy = pltpu.make_async_copy(src, dst, lsem.at[len(local)])
        copy.start()
        local.append(copy)
        return copy

    up_own = upb.at[x, zl, c]
    got_tok = fetch(tokens.at[0], tok.at[cols(0, 16)])
    got_up = fetch(up_w, up_own)
    got_down = fetch(down_w, dwn.at[cols(0, 256), cols(0, 128)])
    got_p = fetch(params.at[0], pbuf)
    got_t = fetch(tracker.at[0], tbuf)
    got_tgt = []
    for rc in range(2):
        for rx in range(4):
            for rz in range(2):
                who = ((x + rx) % 4) * 4 + ((zl + rz) % 2) * 2 + (c + rc) % 2
                src = targets.at[0, :, pl.ds(pl.multiple_of(who * 128, 128), 128)]
                got_tgt.append(fetch(src, tgt.at[:, cols(rc * 1024 + rx * 256 + rz * 128, 128)]))

    barrier = pltpu.get_barrier_semaphore()
    peers = [other_core, off_chip, other_z, beyond, along_x(1), along_x(-1)]
    peers += [along_y(r) for r in range(1, 8)] + [along_z(1), along_z(-1)]
    for peer in peers:
        pl.semaphore_signal(barrier, inc=1, device_id=peer, device_id_type=MESH)
    pl.semaphore_wait(barrier, len(peers))

    sent = []

    def message(src, dst, peer, k, out=None):
        out = k if out is None else out
        return pltpu.make_async_remote_copy(
            src_ref=src, dst_ref=dst, send_sem=ssem.at[out], recv_sem=rsem.at[k],
            device_id=peer, device_id_type=MESH,
        )

    def send(src, dst, peer, k):
        copy = message(src, dst, peer, k)
        copy.start()
        sent.append(copy)

    def arrive(dst, k):
        message(dst, dst, other_core, k).wait_recv()

    def tok_at(r, q):
        return tok.at[cols((r % 8) * 64 + (q % 4) * 16, 16)]

    def dwn_at(r, rx, first=0, rows=256):
        return dwn.at[cols((r % 8) * 256 + first, rows), cols(rx * 256, 256)]

    def tok_steps(way, q):
        return 4 if (q < 2) == (way == 0) else 3

    def tok_step(way, s, q):
        sign = 1 if way == 0 else -1
        send(tok_at(-sign * (s - 1), q), tok_at(-sign * s, q), along_y(sign), TY(way, s, q))

    def tok_wait(way, s, q):
        sign = 1 if way == 0 else -1
        arrive(tok_at(-sign * s, q), TY(way, s, q))

    def dwn_rows(way, s):
        return (0, NEAR) if s < 4 else (NEAR // 2 * way, NEAR // 2)

    def dwn_step(way, s):
        sign = 1 if way == 0 else -1
        part = dwn_rows(way, s)
        send(
            dwn_at(-sign * (s - 1), 0, *part), dwn_at(-sign * s, 0, *part),
            along_y(sign), DY(way, s),
        )

    def dwn_wait(way, s):
        sign = 1 if way == 0 else -1
        arrive(dwn_at(-sign * s, 0, *dwn_rows(way, s)), DY(way, s))

    def dwn_piece(r, z):
        return dwn.at[cols((r % 8) * 256, NEAR), cols(z * 128, 128)]

    def far_at(r, way, s):
        first, n = (NEAR, 256 - NEAR) if s < 4 else (NEAR + (256 - NEAR) // 2 * way, (256 - NEAR) // 2)
        return dwn.at[cols((r % 8) * 256 + first, n), cols(0, 1024)]

    def far_step(way, s):
        sign = 1 if way == 0 else -1
        send(
            far_at(-sign * (s - 1), way, s), far_at(-sign * s, way, s), along_y(sign), EY(way, s)
        )

    def far_wait(s):
        for way in range(2):
            sign = 1 if way == 0 else -1
            arrive(far_at(-sign * s, way, s), EY(way, s))
            if s < 4:
                far_step(way, s + 1)

    def x_first(r):
        send(dwn_at(r, 0, 0, NEAR), dwn_at(r, 3, 0, NEAR), along_x(1), DX(0, r))
        send(dwn_at(r, 0, 0, NEAR), dwn_at(r, 1, 0, NEAR), along_x(-1), DX(1, r))

    def x_pieces(r):
        n = (256 if r == 0 else NEAR) // 2
        return (0, n), (n, n)

    def x_second(r):
        if r == 0:
            for way, rx in ((0, 3), (1, 1)):
                arrive(dwn.at[cols(0, 256), cols(rx * 256, 128)], D0(way))
                arrive(dwn.at[cols(0, 256), cols(rx * 256 + 128, 128)], DX(way, 0))
        else:
            arrive(dwn_at(r, 3, 0, NEAR), DX(0, r))
            arrive(dwn_at(r, 1, 0, NEAR), DX(1, r))
        low, high = x_pieces(r)
        send(dwn_at(r, 3, *low), dwn_at(r, 2, *low), along_x(1), DF(0, r))
        send(dwn_at(r, 1, *high), dwn_at(r, 2, *high), along_x(-1), DF(1, r))

    def core_half(r, rc):
        return dwn.at[cols((r % 8) * 256, 256), cols(rc * 1024, 1024)]

    def x_third(r):
        for way in range(2):
            arrive(dwn_at(r, 2, *x_pieces(r)[way]), DF(way, r))
        send(core_half(r, 0), core_half(r, 1), other_core, DC(r))

    def half_cols(way):
        return cols(way * 1024, 1024)

    def ring_z(ref, base, first):
        own, below, above, far = (ref.at[cols(base + 16 * k, 16)] for k in (0, 3, 1, 2))

        def start():
            send(own, below, along_z(1), first(0, 0))
            send(own, above, along_z(-1), first(0, 1))

        def forward():
            arrive(below, first(0, 0))
            send(below.at[:, half_cols(0)], far.at[:, half_cols(0)], along_z(1), first(1, 0))
            arrive(above, first(0, 1))
            send(above.at[:, half_cols(1)], far.at[:, half_cols(1)], along_z(-1), first(1, 1))

        def finish():
            for way in range(2):
                arrive(far.at[:, half_cols(way)], first(1, way))

        return start, forward, finish

    tok_start, tok_forward, tok_finish = ring_z(tok, 0, TZ)
    got_tok.wait()
    tok_start()
    for way in range(2):
        tok_step(way, 1, 0)
    got_down.wait()
    own_down = dwn.at[cols(0, 256), cols(0, 128)]
    send(own_down, dwn.at[cols(0, 256), cols(128, 128)], other_z, DZ(0))
    for way, rx in ((0, 3), (1, 1)):
        send(own_down, dwn.at[cols(0, 256), cols(rx * 256, 128)], along_x(1 - 2 * way), D0(way))
        send(dwn_piece(0, 0), dwn_piece(2 * way - 1, 0), along_y(1 - 2 * way), DB(way))
    got_up.wait()
    send(up_own, up_own, other_z, UZ(0))
    got_p.wait()
    send(pbuf, pin, other_core, PI(0))
    got_t.wait()
    send(tbuf, tin, other_core, TI(0))

    tok_forward()
    for way in range(2):
        tok_step(way, 1, 3)
        tok_step(way, 1, 1)
    z_down = dwn.at[cols(0, 256), cols(128, 128)]
    arrive(z_down, DZ(0))
    for way, rx in ((0, 3), (1, 1)):
        send(z_down, dwn.at[cols(0, 256), cols(rx * 256 + 128, 128)], along_x(1 - 2 * way), DX(way, 0))
        send(dwn_piece(0, 1), dwn_piece(2 * way - 1, 1), along_y(1 - 2 * way), DY(way, 1))
    arrive(upb.at[x, 1 - zl, c], UZ(0))
    send(upb.at[x, :, c], upb.at[x, :, c], along_x(1), UX(0))
    send(upb.at[x, :, c], upb.at[x, :, c], along_x(-1), UX(1))
    tok_finish()
    for way in range(2):
        tok_step(way, 1, 2)

    low, high = cols(0, 1024), cols(1024, 1024)

    @pl.when(diagonal)
    def _():
        message(pbuf.at[high], prel, other_z, PR(0)).start()
        message(pbuf.at[low], pof.at[low], off_chip, PO(0)).start()

    @pl.when(jnp.logical_not(diagonal))
    def _():
        message(pbuf.at[low], pof.at[low], off_chip, PO(0)).start()
        message(pbuf.at[high], pof.at[high], off_chip, PO(1)).start()

    for copy in got_tgt:
        copy.wait()

    for s in range(1, 5):
        for way in range(2):
            if s == 1:
                arrive(dwn_piece(2 * way - 1, 0), DB(way))
                arrive(dwn_piece(2 * way - 1, 1), DY(way, 1))
            else:
                dwn_wait(way, s)
            if s < 4:
                dwn_step(way, s + 1)
        for r in (8 - s, s)[: 2 if s < 4 else 1]:
            x_first(r)
        for q in (0, 3, 1, 2):
            for way in range(2):
                if s <= tok_steps(way, q):
                    tok_wait(way, s, q)
                    if s < tok_steps(way, q):
                        tok_step(way, s + 1, q)
        if s == 1:
            x_second(0)
            below, above = (x + 3) % 4, (x + 1) % 4
            arrive(upb.at[below, :, c], UX(0))
            send(upb.at[below, 0, c], upb.at[below, 0, c], along_x(1), UF(0))
            arrive(upb.at[above, :, c], UX(1))
            send(upb.at[above, 1, c], upb.at[above, 1, c], along_x(-1), UF(1))
        if s == 2:
            x_third(0)
            for way in range(2):
                far_step(way, 1)
        if s == 3:
            far_wait(1)
            across = (x + 2) % 4
            arrive(upb.at[across, 0, c], UF(0))
            arrive(upb.at[across, 1, c], UF(1))
            send(upb.at[:, :, c], upb.at[:, :, c], other_core, UC(0))
            x_second(7)
            x_second(1)

            @pl.when(jnp.logical_not(diagonal))
            def _():
                arrive(prel, PR(0))
                message(prel, pof.at[high], beyond, PO(1), PO(2)).start()

        if s == 4:
            far_wait(2)
            x_second(6)
            x_second(2)

    @pl.when(diagonal)
    def _():
        message(tbuf, trel, other_z, TR(0)).start()

    @pl.when(jnp.logical_not(diagonal))
    def _():
        message(tbuf, tof, off_chip, TO(0)).start()

    def rows256(i):
        return pl.ds(pl.multiple_of(i * 256, 256), 256)

    arrive(upb.at[:, :, 1 - c], UC(0))

    @pl.loop(0, 2)
    def _(i):
        rows = rows256(i)
        total = jnp.zeros((256, 256), F32)
        for k in range(8):
            total += jnp.dot(
                tok[rows, k * 256 : (k + 1) * 256],
                upb[k // 2, k % 2].reshape(256, 256),
                preferred_element_type=F32,
            )
        upv[rows, :] = total

    def hidden_of(p, weights):
        @pl.loop(0, 2)
        def _(i):
            rows = rows256(i)
            gate = jnp.dot(tok[rows, :], weights[...], preferred_element_type=F32) * scale
            sig = jax.nn.sigmoid(gate)
            up = upv[rows, :]
            hsend[p, rows, :] = (sig * gate * up).astype(BF16)
            fac[p, rows, :] = up * sig * (1.0 + gate * (1.0 - sig))

        for r in FAR_FIRST:
            send(
                hsend.at[p, cols(r * 64, 64)], hall.at[p, :, cols((8 - r) * 256, 256)],
                along_y(r), HI(p, r),
            )
        hall[p, :, 0:256] = hsend[p, 0:64, :]

    hidden_of(0, pbuf)
    far_wait(3)
    x_second(5)
    x_second(3)
    x_third(7)
    x_third(1)
    x_second(4)

    e_off = edge[(a + c + 15) % 16]
    e_in = edge[(a + 16 - c) % 16]
    own = 1.0 - e_off - e_in
    eta = step[0]
    arrive(pin, PI(0))
    arrive(pof.at[low], PO(0))
    arrive(pof.at[high], PO(1))

    @pl.loop(0, 8)
    def _(i):
        rows = rows256(i)
        mixed = own * pbuf[rows, :].astype(F32)
        mixed += e_off * pof[rows, :].astype(F32) + e_in * pin[rows, :].astype(F32)
        fresh[rows, :] = (mixed - eta * tbuf[rows, :].astype(F32)).astype(BF16)

    fresh_copy = pltpu.make_async_copy(fresh, fresh_out.at[0], lsem.at[len(local)])
    fresh_copy.start()
    hidden_of(1, fresh)
    x_third(6)
    x_third(2)
    far_wait(4)
    x_third(5)
    x_third(3)
    x_third(4)

    @pl.when(jnp.logical_not(diagonal))
    def _():
        arrive(trel, TR(0))
        message(trel, tof, beyond, TO(0), TO(1)).start()

    for r in ORDER:
        arrive(core_half(r, 1), DC(r))

    def sum_first(p, way):
        rows, part = cols(32, 16), half_cols(way)
        return psend.at[p, rows, part], pmid.at[p, :, part]

    def sum_second(p, way, half):
        rows, part = cols(16 + 32 * way, 16), half_cols(half)
        return psend.at[p, rows, part], prec.at[p, way, :, part]

    def partial_of(p):
        for r in FAR_FIRST:
            arrive(hall.at[p, :, cols((8 - r) * 256, 256)], HI(p, r))

        @pl.loop(0, 8)
        def _(i):
            part = jnp.dot(hall[p], dwn[:, rows256(i)], preferred_element_type=F32)
            psend[p, :, rows256(i)] = part.astype(BF16)

        for way in range(2):
            send(*sum_first(p, way), along_z(1 - 2 * way), RS(p, 0, way))
        for way in range(2):
            send(*sum_second(p, way, 1 - way), along_z(1 - 2 * way), RS(p, 1, way))

    def middle_of(p):
        for way in range(2):
            arrive(sum_first(p, way)[1], RS(p, 0, way))
            rows, part = cols(16 + 32 * way, 16), half_cols(way)
            both = psend[p, rows, part].astype(F32) + pmid[p, :, part].astype(F32)
            psend[p, rows, part] = both.astype(BF16)
            send(*sum_second(p, way, way), along_z(1 - 2 * way), RS(p, 2, way))

    err_ring = [ring_z(eall.at[p], 0, functools.partial(EG, p)) for p in range(2)]

    def err_of(p):
        total = psend[p, 0:16, :].astype(F32)
        for way in range(2):
            for half in range(2):
                arrive(sum_second(p, way, half)[1], RS(p, 2 if half == way else 1, way))
            total += prec[p, way].astype(F32)
        eall[p, 0:16, :] = (2.0 * (total - tgt[...].astype(F32))).astype(BF16)
        err_ring[p][0]()

    partial_of(0)
    partial_of(1)
    middle_of(0)
    middle_of(1)
    err_of(0)
    err_of(1)
    for p in range(2):
        err_ring[p][1]()

    def back_block(p, r):
        return lax.dot_general(
            eall[p], dwn[pl.ds(pl.multiple_of(r * 256, 256), 256), :],
            (((1,), (1,)), ((), ())), preferred_element_type=F32,
        ).astype(BF16)

    def back_message(p, r):
        rows = pl.ds(pl.multiple_of(r * 64, 64), 64)
        land = pl.ds(pl.multiple_of((8 - r) * 64, 64), 64)
        return message(bsend.at[p, rows], brec.at[p, land], along_y(r), BK(p, 0) + r)

    def back_of(p):
        err_ring[p][2]()

        @pl.loop(0, 7)
        def _(k):
            r = 4 + ((k + 1) // 2) * (1 - 2 * (k % 2))
            bsend[p, pl.ds(pl.multiple_of(r * 64, 64), 64), :] = back_block(p, r)
            back_message(p, r).start()

        brec[p, 0:64, :] = back_block(p, 0)

    back_of(0)
    back_of(1)

    arrive(tin, TI(0))
    arrive(tof, TO(0))

    @pl.loop(0, 8)
    def _(i):
        rows = rows256(i)
        turned[rows, :] = tok[:, rows].T
        mixed = own * tbuf[rows, :].astype(F32)
        mixed += e_off * tof[rows, :].astype(F32) + e_in * tin[rows, :].astype(F32)
        mixed_y[rows, :] = mixed

    for p in range(2):

        @pl.loop(1, 8)
        def _(r):
            land = pl.ds(pl.multiple_of((8 - r) * 64, 64), 64)
            message(brec.at[p, land], brec.at[p, land], other_core, BK(p, 0) + r).wait_recv()

    dd[...] = (
        brec[1].astype(F32) * fac[1] - brec[0].astype(F32) * fac[0]
    ).astype(BF16)

    @pl.loop(0, 8)
    def _(i):
        rows = rows256(i)
        change = jnp.dot(turned[rows, :], dd[...], preferred_element_type=F32)
        trk[rows, :] = (mixed_y[rows, :] + change * scale).astype(BF16)
        pltpu.make_async_copy(trk.at[rows], track_out.at[0, rows], lsem.at[len(local) + 1]).start()

    for copy in sent:
        copy.wait_send()

    @pl.when(diagonal)
    def _():
        message(pbuf.at[high], prel, other_z, PR(0)).wait_send()
        message(pbuf.at[low], pof.at[low], off_chip, PO(0)).wait_send()
        message(tbuf, trel, other_z, TR(0)).wait_send()

    @pl.when(jnp.logical_not(diagonal))
    def _():
        message(pbuf.at[low], pof.at[low], off_chip, PO(0)).wait_send()
        message(pbuf.at[high], pof.at[high], off_chip, PO(1)).wait_send()
        message(prel, pof.at[high], beyond, PO(1), PO(2)).wait_send()
        message(tbuf, tof, off_chip, TO(0)).wait_send()
        message(trel, tof, beyond, TO(0), TO(1)).wait_send()

    for p in range(2):

        @pl.loop(1, 8)
        def _(r):
            back_message(p, r).wait_send()

    fresh_copy.wait()
    pltpu.make_async_copy(trk, track_out.at[0], lsem.at[len(local) + 1]).wait()


def on_device(tokens, targets, params, tracker, up_weight, down_weight, edge_weight, step_size):
    hbm = pl.BlockSpec(memory_space=pltpu.HBM)
    smem = pl.BlockSpec(memory_space=pltpu.SMEM)
    block = pltpu.VMEM((2048, 256), BF16)
    out = jax.ShapeDtypeStruct(params.shape, BF16)
    return pl.pallas_call(
        kernel,
        out_shape=(out, out),
        in_specs=[smem, smem] + [hbm] * 6,
        out_specs=(hbm, hbm),
        scratch_shapes=[
            pltpu.VMEM((512, 2048), BF16),
            pltpu.VMEM((16, 2048), BF16),
            block, block, block, block, block, block, block,
            pltpu.VMEM((4, 2, 2, 128, 256), BF16),
            pltpu.VMEM((2048, 2048), BF16),
            pltpu.VMEM((512, 256), F32),
            pltpu.VMEM((2, 512, 256), F32),
            pltpu.VMEM((2, 512, 256), BF16),
            pltpu.VMEM((2, 64, 2048), BF16),
            pltpu.VMEM((2, 64, 2048), BF16),
            pltpu.VMEM((2, 16, 2048), BF16),
            pltpu.VMEM((2, 2, 16, 2048), BF16),
            pltpu.VMEM((2, 64, 2048), BF16),
            pltpu.VMEM((2, 512, 256), BF16),
            pltpu.VMEM((2, 512, 256), BF16),
            pltpu.VMEM((512, 256), BF16),
            block,
            pltpu.VMEM((1024, 256), BF16),
            block,
            pltpu.VMEM((2048, 512), BF16),
            pltpu.VMEM((2048, 256), F32),
            pltpu.SemaphoreType.DMA((SEMS,)),
            pltpu.SemaphoreType.DMA((SEMS,)),
            pltpu.SemaphoreType.DMA((24,)),
        ],
        compiler_params=pltpu.CompilerParams(
            collective_id=0, has_side_effects=True, vmem_limit_bytes=56 * 1024 * 1024
        ),
    )(edge_weight, step_size, tokens, targets, params, tracker, up_weight, down_weight)


def solution(mesh):
    in_specs = (
        P("agent", "tp", None),
        P("agent", "tp", None),
        P("agent", None, "tp"),
        P("agent", None, "tp"),
        P("agent", "tp"),
        P("tp", "agent"),
        P(),
        P(),
    )
    out_specs = (P("agent", None, "tp"), P("agent", None, "tp"))
    return jax.shard_map(
        on_device, mesh=mesh, in_specs=in_specs, out_specs=out_specs, check_vma=False
    )
```

```python
import functools
import math

import jax
import jax.numpy as jnp
from jax import lax
from jax.experimental import pallas as pl
from jax.experimental.pallas import tpu as pltpu
from jax.sharding import PartitionSpec as P

MESH = pl.DeviceIdType.MESH
BF16 = jnp.bfloat16
F32 = jnp.float32
ORDER = (0, 7, 1, 6, 2, 5, 3, 4)
NEAR = 224
PARTS = 4
FAR_FIRST = (4, 3, 5, 2, 6, 1, 7)


class Plan:
    def __init__(self):
        self.count = 0

    def take(self, *shape):
        size = 1
        for n in shape:
            size *= n
        base = self.count
        self.count += size

        def number(*index):
            flat = 0
            for i, n in zip(index, shape):
                flat = flat * n + i
            return base + flat

        return number


plan = Plan()
TZ, TY = plan.take(3), plan.take(2, 2, 7)
UZ, UX, UF, UC = plan.take(1), plan.take(2), plan.take(1), plan.take(1)
DZ, DB, D0 = plan.take(1), plan.take(2), plan.take(2)
DY, EY = plan.take(2, 4), plan.take(2, 4)
DX, DF, DC = plan.take(2, 8), plan.take(8), plan.take(8)
PI, PO, TI, TO, PR = plan.take(1), plan.take(3), plan.take(1), plan.take(1), plan.take(2)
HI, BK = plan.take(2), plan.take(2)
RS, EG = plan.take(2, 3), plan.take(2, 3)
SEMS = plan.count
SENDS = 8
BLOCK_SENT, ON_SENT, STRAIGHT_SENT, BACK_SENT = range(SENDS, SENDS + 4)

def kernel(
    edge, step, tokens, targets, params, tracker, up_w, down_w, fresh_out, dd_out, turned_out, mixed_out,
    tok, tgt, pbuf, tbuf, pin, pof, tin, tof, fresh, upb, dwn, upv, fac, hsend, hall,
    psend, pmid, prec, eall, bsend, brec, dd, prel, turned, mixed_y, ssem, rsem, lsem,
):
    a = lax.axis_index("agent")
    t = lax.axis_index("tp")
    x, zl, c = a // 4, (a // 2) % 2, a % 2
    zh, y = t // 8, t % 8
    scale = 2048.0 ** -0.5

    def along_y(r):
        return (a, zh * 8 + (y + r + 8) % 8)

    def along_z(q):
        return (a, ((zh + q + 4) % 4) * 8 + y)

    def along_x(r):
        return ((a + 4 * r + 16) % 16, t)

    other_core = (a + 1 - 2 * c, t)
    off_chip = ((a + 2 * c + 15) % 16, t)
    other_z = (a + 2 - 4 * zl, t)
    onward = ((a + 8 * c + 12) % 16, t)
    corner = (4 * x + 3 - (a % 4), t)
    diagonal = c == zl

    def cols(first, n):
        return pl.ds(first, n)

    def fetch(src, dst, k):
        copy = pltpu.make_async_copy(src, dst, lsem.at[k])
        copy.start()
        return copy

    up_own = upb.at[x, zl, c]
    got_tok = fetch(tokens.at[0], tok.at[cols(0, 16)], 0)
    got_up = fetch(up_w, up_own, 1)
    got_down = fetch(down_w, dwn.at[cols(0, 256), cols(0, 128)], 2)
    got_p = fetch(params.at[0], pbuf, 3)
    got_t = fetch(tracker.at[0], tbuf, 4)
    for rc in range(2):
        for rx in range(4):
            for rz in range(2):
                who = ((x + rx) % 4) * 4 + ((zl + rz) % 2) * 2 + (c + rc) % 2
                src = targets.at[0, :, pl.ds(pl.multiple_of(who * 128, 128), 128)]
                fetch(src, tgt.at[:, cols(rc * 1024 + rx * 256 + rz * 128, 128)], 5)

    barrier = pltpu.get_barrier_semaphore()
    peers = [other_core, off_chip, other_z, corner, along_x(1), along_x(-1)]
    peers += [along_y(r) for r in range(1, 8)] + [along_z(1), along_z(-1)]
    for peer in peers:
        pl.semaphore_signal(barrier, inc=1, device_id=peer, device_id_type=MESH)
    pl.semaphore_wait(barrier, len(peers))

    sent = [0]

    def message(src, dst, peer, k, out=0):
        return pltpu.make_async_remote_copy(
            src_ref=src, dst_ref=dst, send_sem=ssem.at[out], recv_sem=rsem.at[k],
            device_id=peer, device_id_type=MESH,
        )

    def send(src, dst, peer, k):
        message(src, dst, peer, k, len(sent) - 1).start()
        sent[-1] += math.prod(src.shape) * 2
        if sent[-1] >= 5 << 19 and sent[-1] % (1 << 15) == 0:
            sent.append(0)

    def arrive(dst, k):
        message(dst, dst, other_core, k).wait_recv()

    def all_sent(nbytes, out):
        rows = dwn.at[cols(0, nbytes // 2048), cols(0, 1024)]
        message(rows, rows, other_core, 0, out).wait_send()

    def tok_at(r, q):
        return tok.at[cols((r % 8) * 64 + (q % 4) * 16, 16)]

    def dwn_at(r, rx, first=0, rows=256):
        return dwn.at[cols((r % 8) * 256 + first, rows), cols(rx * 256, 256)]

    def tok_steps(way, q):
        return 4 if (q < 2) == (way == 0) else 3

    def tok_sem(way, s, q):
        pair, rank = divmod(q, 2)
        if pair == way:
            return TY(way, rank, s - 1)
        return TY(way, rank, 3 + s)

    def tok_step(way, s, q):
        sign = 1 if way == 0 else -1
        send(tok_at(-sign * (s - 1), q), tok_at(-sign * s, q), along_y(sign), tok_sem(way, s, q))

    def tok_wait(way, s, q):
        sign = 1 if way == 0 else -1
        arrive(tok_at(-sign * s, q), tok_sem(way, s, q))

    def dwn_rows(way, s):
        return (0, NEAR) if s < 4 else (NEAR // 2 * way, NEAR // 2)

    def dwn_step(way, s):
        sign = 1 if way == 0 else -1
        part = dwn_rows(way, s)
        send(
            dwn_at(-sign * (s - 1), 0, *part), dwn_at(-sign * s, 0, *part),
            along_y(sign), DY(way, s - 1),
        )

    def dwn_wait(way, s):
        sign = 1 if way == 0 else -1
        arrive(dwn_at(-sign * s, 0, *dwn_rows(way, s)), DY(way, s - 1))

    def dwn_piece(r, z):
        return dwn.at[cols((r % 8) * 256, NEAR), cols(z * 128, 128)]

    def far_at(r, way, s):
        first, n = (NEAR, 256 - NEAR) if s < 4 else (NEAR + (256 - NEAR) // 2 * way, (256 - NEAR) // 2)
        return dwn.at[cols((r % 8) * 256 + first, n), cols(0, 1024)]

    def far_step(way, s):
        sign = 1 if way == 0 else -1
        send(
            far_at(-sign * (s - 1), way, s), far_at(-sign * s, way, s), along_y(sign), EY(way, s - 1)
        )

    def far_wait(s):
        for way in range(2):
            sign = 1 if way == 0 else -1
            arrive(far_at(-sign * s, way, s), EY(way, s - 1))
            if s < 4:
                far_step(way, s + 1)

    def x_first(r):
        send(dwn_at(r, 0, 0, NEAR), dwn_at(r, 3, 0, NEAR), along_x(1), DX(0, r))
        send(dwn_at(r, 0, 0, NEAR), dwn_at(r, 1, 0, NEAR), along_x(-1), DX(1, r))

    def x_pieces(r):
        n = (256 if r == 0 else NEAR) // 2
        return (0, n), (n, n)

    def x_second(r):
        if r == 0:
            for way, rx in ((0, 3), (1, 1)):
                arrive(dwn.at[cols(0, 256), cols(rx * 256, 128)], D0(way))
                arrive(dwn.at[cols(0, 256), cols(rx * 256 + 128, 128)], DX(way, 0))
        else:
            arrive(dwn_at(r, 3, 0, NEAR), DX(0, r))
            arrive(dwn_at(r, 1, 0, NEAR), DX(1, r))
        low, high = x_pieces(r)
        send(dwn_at(r, 3, *low), dwn_at(r, 2, *low), along_x(1), DF(r))
        send(dwn_at(r, 1, *high), dwn_at(r, 2, *high), along_x(-1), DF(r))

    def core_half(r, rc):
        return dwn.at[cols((r % 8) * 256, 256), cols(rc * 1024, 1024)]

    def x_third(r):
        arrive(dwn_at(r, 2, 0, 256 if r == 0 else NEAR), DF(r))
        send(core_half(r, 0), core_half(r, 1), other_core, DC(r))

    def half_cols(way):
        return cols(way * 1024, 1024)

    def ring_z(ref, base, first):
        own, below, above, far = (ref.at[cols(base + 16 * k, 16)] for k in (0, 3, 1, 2))

        def start():
            send(own, below, along_z(1), first(0))
            send(own, above, along_z(-1), first(1))

        def forward():
            arrive(below, first(0))
            send(below.at[:, half_cols(0)], far.at[:, half_cols(0)], along_z(1), first(2))
            arrive(above, first(1))
            send(above.at[:, half_cols(1)], far.at[:, half_cols(1)], along_z(-1), first(2))

        def finish():
            arrive(far, first(2))

        return start, forward, finish

    tok_start, tok_forward, tok_finish = ring_z(tok, 0, TZ)
    got_down.wait()
    own_down = dwn.at[cols(0, 256), cols(0, 128)]
    send(own_down, dwn.at[cols(0, 256), cols(128, 128)], other_z, DZ(0))
    got_tok.wait()
    tok_start()
    for way in range(2):
        tok_step(way, 1, 0)
    for way, rx in ((0, 3), (1, 1)):
        send(own_down, dwn.at[cols(0, 256), cols(rx * 256, 128)], along_x(1 - 2 * way), D0(way))
        send(dwn_piece(0, 0), dwn_piece(2 * way - 1, 0), along_y(1 - 2 * way), DB(way))
    got_up.wait()
    send(up_own, up_own, other_z, UZ(0))
    got_p.wait()
    low, quarters = cols(0, 1024), (cols(1024, 512), cols(1536, 512))

    def onward_half(k):
        return message(pbuf.at[quarters[k]], prel.at[cols(512 * k, 512)], onward, PR(k), ON_SENT)

    def corner_half(k):
        return message(prel.at[cols(512 * k, 512)], pof.at[quarters[k]], corner, PO(1 + k), ON_SENT)

    def straight_half(k):
        return message(pbuf.at[quarters[k]], pof.at[quarters[k]], off_chip, PO(1 + k), STRAIGHT_SENT)

    direct_half = message(pbuf.at[low], pof.at[low], off_chip, PO(0), BLOCK_SENT)

    @pl.when(diagonal)
    def _():
        onward_half(0).start()

    send(pbuf, pin, other_core, PI(0))
    got_t.wait()
    send(tbuf, tin, other_core, TI(0))

    z_down = dwn.at[cols(0, 256), cols(128, 128)]
    arrive(z_down, DZ(0))
    for way, rx in ((0, 3), (1, 1)):
        send(dwn_piece(0, 1), dwn_piece(2 * way - 1, 1), along_y(1 - 2 * way), DY(way, 0))
        send(z_down, dwn.at[cols(0, 256), cols(rx * 256 + 128, 128)], along_x(1 - 2 * way), DX(way, 0))
    tok_forward()
    for way in range(2):
        tok_step(way, 1, 3)
        tok_step(way, 1, 1)

    arrive(upb.at[x, 1 - zl, c], UZ(0))
    send(upb.at[x, :, c], upb.at[x, :, c], along_x(1), UX(0))
    send(upb.at[x, :, c], upb.at[x, :, c], along_x(-1), UX(1))

    @pl.when(jnp.logical_not(diagonal))
    def _():
        direct_half.start()
        straight_half(0).start()
        straight_half(1).start()

    tok_finish()
    for way in range(2):
        tok_step(way, 1, 2)
    pltpu.make_async_copy(tgt, tgt, lsem.at[5]).wait()

    def down(s):
        for way in range(2):
            if s == 1:
                arrive(dwn_piece(2 * way - 1, 0), DB(way))
                arrive(dwn_piece(2 * way - 1, 1), DY(way, 0))
            else:
                dwn_wait(way, s)
            if s < 4:
                dwn_step(way, s + 1)
        if s == 1:
            x_second(0)
        for r in (8 - s, s)[: 2 if s < 4 else 1]:
            x_first(r)

    def token(s, *pieces):
        for q in pieces:
            for way in range(2):
                if s <= tok_steps(way, q):
                    tok_wait(way, s, q)
                    if s < tok_steps(way, q):
                        tok_step(way, s + 1, q)

    down(1)
    token(1, 0, 3)
    down(2)
    whole_t = message(tbuf, tof, off_chip, TO(0), BLOCK_SENT)

    @pl.when(jnp.logical_not(diagonal))
    def _():
        whole_t.start()

    def track_piece(k):
        rows = cols(1024 * k, 1024)

        @pl.when(diagonal)
        def _():
            message(tbuf.at[rows], tof.at[rows], off_chip, TO(0), BLOCK_SENT).start()

    below, above, across = (x + 3) % 4, (x + 1) % 4, (x + 2) % 4
    arrive(upb.at[below, :, c], UX(0))
    send(upb.at[below, 0, c], upb.at[below, 0, c], along_x(1), UF(0))
    arrive(upb.at[above, :, c], UX(1))
    send(upb.at[above, 1, c], upb.at[above, 1, c], along_x(-1), UF(0))
    token(1, 1, 2)

    @pl.when(diagonal)
    def _():
        onward_half(1).start()
        arrive(prel.at[cols(0, 512)], PR(0))
        corner_half(0).start()

    token(2, 0)
    x_third(0)
    for way in range(2):
        far_step(way, 1)
    down(3)

    @pl.when(diagonal)
    def _():
        direct_half.start()

    token(2, 3, 1)
    x_second(7)
    x_second(1)
    down(4)
    token(2, 2)
    far_wait(1)

    @pl.when(diagonal)
    def _():
        arrive(prel.at[cols(512, 512)], PR(1))
        corner_half(1).start()

    token(3, 0, 3)
    x_second(6)
    x_second(2)
    arrive(upb.at[across, :, c], UF(0))
    send(upb.at[:, :, c], upb.at[:, :, c], other_core, UC(0))
    token(3, 1, 2)
    far_wait(2)
    x_third(7)
    x_third(1)
    token(4, 0, 3, 1, 2)
    far_wait(3)

    def rows256(i):
        return pl.ds(pl.multiple_of(i * 256, 256), 256)

    arrive(upb.at[:, :, 1 - c], UC(0))

    def hidden_half(p, weights, half):
        rows = cols(256 * half, 256)
        if p == 0:
            sums = jnp.zeros((256, 256), F32)
            for k in range(8):
                sums += jnp.dot(
                    tok[rows, k * 256 : (k + 1) * 256],
                    upb[k // 2, k % 2].reshape(256, 256),
                    preferred_element_type=F32,
                )
            upv[rows, :] = sums
        gate = jnp.dot(tok[rows, :], weights[...], preferred_element_type=F32) * scale
        sig = jax.nn.sigmoid(gate)
        up = upv[rows, :]
        hsend[p, rows, :] = (sig * gate * up).astype(BF16)
        fac[p, rows, :] = up * sig * (1.0 + gate * (1.0 - sig))

    def hidden_of(p, weights):
        for half, blocks in ((1, (4, 5, 6, 7)), (0, (3, 2, 1))):
            hidden_half(p, weights, half)
            for r in blocks:
                send(
                    hsend.at[p, cols(r * 64, 64)], hall.at[p, :, cols((8 - r) * 256, 256)],
                    along_y(r), HI(p),
                )
        hall[p, :, 0:256] = hsend[p, 0:64, :]

    hidden_of(0, pbuf)
    track_piece(0)
    x_second(5)
    x_second(3)
    x_second(4)
    x_third(6)
    x_third(2)

    e_off = edge[(a + c + 15) % 16]
    e_in = edge[(a + 16 - c) % 16]
    own = 1.0 - e_off - e_in
    eta = step[0]
    arrive(pin, PI(0))
    arrive(pof.at[low], PO(0))
    for k in range(2):
        arrive(pof.at[quarters[k]], PO(1 + k))

    @pl.loop(0, 8)
    def _(i):
        rows = rows256(i)
        mixed = own * pbuf[rows, :].astype(F32)
        mixed += e_off * pof[rows, :].astype(F32) + e_in * pin[rows, :].astype(F32)
        fresh[rows, :] = (mixed - eta * tbuf[rows, :].astype(F32)).astype(BF16)

    fresh_copy = pltpu.make_async_copy(fresh, fresh_out.at[0], lsem.at[6])
    fresh_copy.start()
    hidden_of(1, fresh)
    far_wait(4)
    x_third(5)
    x_third(3)
    x_third(4)

    def sum_first(p, way):
        rows, part = cols(32, 16), half_cols(way)
        return psend.at[p, rows, part], pmid.at[p, :, part]

    def sum_second(p, way, half):
        rows, part = cols(16 + 32 * way, 16), half_cols(half)
        return psend.at[p, rows, part], prec.at[p, way, :, part]

    def hidden_wait(p):
        arrive(hall.at[p, :, cols(256, 1792)], HI(p))

    def partial_of(p):
        hidden_wait(p)
        for half in range(2):
            if p == 0 and half == 1:
                for r in ORDER:
                    arrive(core_half(r, 1), DC(r))

            @pl.loop(4 * half, 4 * half + 4)
            def _(i):
                part = jnp.dot(hall[p], dwn[:, rows256(i)], preferred_element_type=F32)
                psend[p, :, rows256(i)] = part.astype(BF16)

            send(*sum_first(p, half), along_z(1 - 2 * half), RS(p, half))
            send(*sum_second(p, 1 - half, half), along_z(2 * half - 1), RS(p, 2))

    def middle_of(p):
        for way in range(2):
            arrive(sum_first(p, way)[1], RS(p, way))
            rows, part = cols(16 + 32 * way, 16), half_cols(way)
            both = psend[p, rows, part].astype(F32) + pmid[p, :, part].astype(F32)
            psend[p, rows, part] = both.astype(BF16)
            send(*sum_second(p, way, way), along_z(1 - 2 * way), RS(p, 2))

    err_ring = [ring_z(eall.at[p], 0, functools.partial(EG, p)) for p in range(2)]

    def err_of(p):
        out = psend[p, 0:16, :].astype(F32)
        arrive(prec.at[p], RS(p, 2))
        for way in range(2):
            out += prec[p, way].astype(F32)
        eall[p, 0:16, :] = (2.0 * (out - tgt[...].astype(F32))).astype(BF16)
        err_ring[p][0]()

    partial_of(0)
    partial_of(1)
    middle_of(0)
    middle_of(1)
    err_of(0)
    err_of(1)
    for p in range(2):
        err_ring[p][1]()
    track_piece(1)

    def back_block(p, r):
        return lax.dot_general(
            eall[p], dwn[pl.ds(pl.multiple_of(r * 256, 256), 256), :],
            (((1,), (1,)), ((), ())), preferred_element_type=F32,
        ).astype(BF16)

    def back_message(p, r):
        rows = pl.ds(pl.multiple_of(r * 64, 64), 64)
        land = pl.ds(pl.multiple_of((8 - r) * 64, 64), 64)
        return message(bsend.at[p, rows], brec.at[p, land], along_y(r), BK(p), BACK_SENT)

    def back_of(p):
        err_ring[p][2]()

        @pl.loop(0, 7)
        def _(k):
            r = 4 + ((k + 1) // 2) * (1 - 2 * (k % 2))
            bsend[p, pl.ds(pl.multiple_of(r * 64, 64), 64), :] = back_block(p, r)
            back_message(p, r).start()

        brec[p, 0:64, :] = back_block(p, 0)

    back_of(0)
    back_of(1)

    arrive(tin, TI(0))
    arrive(tof, TO(0))

    def prepare():
        @pl.loop(0, 8)
        def _(i):
            rows = rows256(i)
            turned[rows, :] = tok[:, rows].T
            mixed = own * tbuf[rows, :].astype(F32)
            mixed += e_off * tof[rows, :].astype(F32) + e_in * tin[rows, :].astype(F32)
            mixed_y[rows, :] = mixed

    prepare()
    turned_copy = pltpu.make_async_copy(turned, turned_out, lsem.at[7])
    mixed_copy = pltpu.make_async_copy(mixed_y, mixed_out, lsem.at[0])
    turned_copy.start()
    mixed_copy.start()

    for p in range(2):
        arrive(brec.at[p, cols(64, 448)], BK(p))

    dd[...] = (
        brec[1].astype(F32) * fac[1] - brec[0].astype(F32) * fac[0]
    ).astype(BF16)

    dd_copy = pltpu.make_async_copy(dd, dd_out, lsem.at[5])
    dd_copy.start()

    for g, nbytes in enumerate(sent):
        if nbytes:
            all_sent(nbytes, g)
    all_sent(3 << 19, BLOCK_SENT)
    all_sent(14 << 15, BACK_SENT)

    @pl.when(diagonal)
    def _():
        all_sent(1 << 20, ON_SENT)

    @pl.when(jnp.logical_not(diagonal))
    def _():
        all_sent(1 << 19, STRAIGHT_SENT)

    fresh_copy.wait()
    turned_copy.wait()
    mixed_copy.wait()
    dd_copy.wait()


def last_kernel(
    dd_in, turned_in, mixed_in, fresh_in, fresh_out, track_out,
    dd, turned, mixed, fresh, track, sem, out_sem,
):
    first = pltpu.make_async_copy(dd_in, dd, sem.at[0])
    first.start()
    pieces = []
    for k in range(PARTS):
        rows = pl.ds(k * (2048 // PARTS), 2048 // PARTS)
        a = pltpu.make_async_copy(turned_in.at[rows], turned.at[rows], sem.at[1 + 2 * k])
        b = pltpu.make_async_copy(mixed_in.at[rows], mixed.at[rows], sem.at[2 + 2 * k])
        a.start()
        b.start()
        pieces.append((rows, a, b))
    middle = pltpu.make_async_copy(fresh_in, fresh, sem.at[1 + 2 * PARTS])
    middle.start()
    done = []
    first.wait()
    for k, (rows, a, b) in enumerate(pieces):
        a.wait()
        b.wait()
        change = jnp.dot(turned[rows, :], dd[...], preferred_element_type=F32)
        track[rows, :] = (mixed[rows, :] + change * 2048.0 ** -0.5).astype(BF16)
        done.append(pltpu.make_async_copy(track.at[rows], track_out.at[0, rows], out_sem.at[k]))
        done[-1].start()
        if k == PARTS - 2:
            middle.wait()
            done.append(pltpu.make_async_copy(fresh, fresh_out, out_sem.at[PARTS]))
            done[-1].start()
    for copy in done:
        copy.wait()


def on_device(tokens, targets, params, tracker, up_weight, down_weight, edge_weight, step_size):
    hbm = pl.BlockSpec(memory_space=pltpu.HBM)
    smem = pl.BlockSpec(memory_space=pltpu.SMEM)
    block = pltpu.VMEM((2048, 256), BF16)
    out = jax.ShapeDtypeStruct(params.shape, BF16)
    fresh, dd, turned, mixed = pl.pallas_call(
        kernel,
        out_shape=(
            out,
            jax.ShapeDtypeStruct((512, 256), BF16),
            jax.ShapeDtypeStruct((2048, 512), BF16),
            jax.ShapeDtypeStruct((2048, 256), F32),
        ),
        in_specs=[smem, smem] + [hbm] * 6,
        out_specs=(hbm, hbm, hbm, hbm),
        scratch_shapes=[
            pltpu.VMEM((512, 2048), BF16),
            pltpu.VMEM((16, 2048), BF16),
            block, block, block, block, block, block, block,
            pltpu.VMEM((4, 2, 2, 128, 256), BF16),
            pltpu.VMEM((2048, 2048), BF16),
            pltpu.VMEM((512, 256), F32),
            pltpu.VMEM((2, 512, 256), F32),
            pltpu.VMEM((2, 512, 256), BF16),
            pltpu.VMEM((2, 64, 2048), BF16),
            pltpu.VMEM((2, 64, 2048), BF16),
            pltpu.VMEM((2, 16, 2048), BF16),
            pltpu.VMEM((2, 2, 16, 2048), BF16),
            pltpu.VMEM((2, 64, 2048), BF16),
            pltpu.VMEM((2, 512, 256), BF16),
            pltpu.VMEM((2, 512, 256), BF16),
            pltpu.VMEM((512, 256), BF16),
            pltpu.VMEM((1024, 256), BF16),
            pltpu.VMEM((2048, 512), BF16),
            pltpu.VMEM((2048, 256), F32),
            pltpu.SemaphoreType.DMA((SENDS + 4,)),
            pltpu.SemaphoreType.DMA((SEMS,)),
            pltpu.SemaphoreType.DMA((8,)),
        ],
        compiler_params=pltpu.CompilerParams(
            collective_id=0, has_side_effects=True, vmem_limit_bytes=56 * 1024 * 1024
        ),
    )(edge_weight, step_size, tokens, targets, params, tracker, up_weight, down_weight)
    return pl.pallas_call(
        last_kernel,
        out_shape=(out, out),
        in_specs=[hbm] * 4,
        out_specs=(hbm, hbm),
        scratch_shapes=[
            pltpu.VMEM((512, 256), BF16),
            pltpu.VMEM((2048, 512), BF16),
            pltpu.VMEM((2048, 256), F32),
            pltpu.VMEM((1, 2048, 256), BF16),
            block,
            pltpu.SemaphoreType.DMA((2 + 2 * PARTS,)),
            pltpu.SemaphoreType.DMA((1 + PARTS,)),
        ],
    )(dd, turned, mixed, fresh)


def solution(mesh):
    in_specs = (
        P("agent", "tp", None),
        P("agent", "tp", None),
        P("agent", None, "tp"),
        P("agent", None, "tp"),
        P("agent", "tp"),
        P("tp", "agent"),
        P(),
        P(),
    )
    out_specs = (P("agent", None, "tp"), P("agent", None, "tp"))
    return jax.shard_map(
        on_device, mesh=mesh, in_specs=in_specs, out_specs=out_specs, check_vma=False
    )
```

```python
import functools
import math

import jax
import jax.numpy as jnp
from jax import lax
from jax.experimental import pallas as pl
from jax.experimental.pallas import tpu as pltpu
from jax.sharding import PartitionSpec as P

MESH = pl.DeviceIdType.MESH
BF16 = jnp.bfloat16
F32 = jnp.float32
ORDER = (0, 7, 1, 6, 2, 5, 3, 4)
NEAR = 224
PARTS = 4
FAR_FIRST = (4, 3, 5, 2, 6, 1, 7)


class Plan:
    def __init__(self):
        self.count = 0

    def take(self, *shape):
        size = 1
        for n in shape:
            size *= n
        base = self.count
        self.count += size

        def number(*index):
            flat = 0
            for i, n in zip(index, shape):
                flat = flat * n + i
            return base + flat

        return number


plan = Plan()
TZ, TY = plan.take(3), plan.take(2, 2, 7)
UZ, UX, UF, UC = plan.take(1), plan.take(2), plan.take(1), plan.take(1)
DZ, DB, D0 = plan.take(1), plan.take(2), plan.take(2)
DY, EY = plan.take(2, 4), plan.take(2, 4)
DX, DF, DC = plan.take(2, 8), plan.take(8), plan.take(8)
PI, PO, TI, TO, PR = plan.take(1), plan.take(4), plan.take(1), plan.take(1), plan.take(3)
HI, BK = plan.take(2), plan.take(2)
RS, EG = plan.take(2, 3), plan.take(2, 3)
SEMS = plan.count
SENDS = 8
BLOCK_SENT, ON_SENT, STRAIGHT_SENT, BACK_SENT = range(SENDS, SENDS + 4)

def kernel(
    edge, step, tokens, targets, params, tracker, up_w, down_w, fresh_out, dd_out, turned_out, mixed_out,
    tok, tgt, pbuf, tbuf, pin, pof, tin, tof, fresh, upb, dwn, upv, fac, hsend, hall,
    psend, pmid, prec, eall, bsend, brec, dd, prel, turned, mixed_y, ssem, rsem, lsem,
):
    a = lax.axis_index("agent")
    t = lax.axis_index("tp")
    x, zl, c = a // 4, (a // 2) % 2, a % 2
    zh, y = t // 8, t % 8
    scale = 2048.0 ** -0.5

    def along_y(r):
        return (a, zh * 8 + (y + r + 8) % 8)

    def along_z(q):
        return (a, ((zh + q + 4) % 4) * 8 + y)

    def along_x(r):
        return ((a + 4 * r + 16) % 16, t)

    other_core = (a + 1 - 2 * c, t)
    off_chip = ((a + 2 * c + 15) % 16, t)
    other_z = (a + 2 - 4 * zl, t)
    onward = ((a + 8 * c + 12) % 16, t)
    corner = (4 * x + 3 - (a % 4), t)
    diagonal = c == zl

    def cols(first, n):
        return pl.ds(first, n)

    barrier = pltpu.get_barrier_semaphore()
    peers = [other_core, off_chip, other_z, corner, along_x(1), along_x(-1)]
    peers += [along_y(r) for r in range(1, 8)] + [along_z(1), along_z(-1)]
    for peer in peers:
        pl.semaphore_signal(barrier, inc=1, device_id=peer, device_id_type=MESH)

    def fetch(src, dst, k):
        copy = pltpu.make_async_copy(src, dst, lsem.at[k])
        copy.start()
        return copy

    up_own = upb.at[x, zl, c]
    got_tok = fetch(tokens.at[0], tok.at[cols(0, 16)], 0)
    got_up = fetch(up_w, up_own, 1)
    got_down = fetch(down_w, dwn.at[cols(0, 256), cols(0, 128)], 2)
    got_p = fetch(params.at[0], pbuf, 3)
    got_t = fetch(tracker.at[0], tbuf, 4)
    for rc in range(2):
        for rx in range(4):
            for rz in range(2):
                who = ((x + rx) % 4) * 4 + ((zl + rz) % 2) * 2 + (c + rc) % 2
                src = targets.at[0, :, pl.ds(pl.multiple_of(who * 128, 128), 128)]
                fetch(src, tgt.at[:, cols(rc * 1024 + rx * 256 + rz * 128, 128)], 5)

    pl.semaphore_wait(barrier, len(peers))

    sent = [0]

    def message(src, dst, peer, k, out=0):
        return pltpu.make_async_remote_copy(
            src_ref=src, dst_ref=dst, send_sem=ssem.at[out], recv_sem=rsem.at[k],
            device_id=peer, device_id_type=MESH,
        )

    def send(src, dst, peer, k):
        message(src, dst, peer, k, len(sent) - 1).start()
        sent[-1] += math.prod(src.shape) * 2
        if sent[-1] >= 5 << 19 and sent[-1] % (1 << 15) == 0:
            sent.append(0)

    def arrive(dst, k):
        message(dst, dst, other_core, k).wait_recv()

    def all_sent(nbytes, out):
        rows = dwn.at[cols(0, nbytes // 2048), cols(0, 1024)]
        message(rows, rows, other_core, 0, out).wait_send()

    def tok_at(r, q):
        return tok.at[cols((r % 8) * 64 + (q % 4) * 16, 16)]

    def dwn_at(r, rx, first=0, rows=256):
        return dwn.at[cols((r % 8) * 256 + first, rows), cols(rx * 256, 256)]

    def tok_steps(way, q):
        return 4 if (q < 2) == (way == 0) else 3

    def tok_sem(way, s, q):
        pair, rank = divmod(q, 2)
        if pair == way:
            return TY(way, rank, s - 1)
        return TY(way, rank, 3 + s)

    def tok_step(way, s, q):
        sign = 1 if way == 0 else -1
        send(tok_at(-sign * (s - 1), q), tok_at(-sign * s, q), along_y(sign), tok_sem(way, s, q))

    def tok_wait(way, s, q):
        sign = 1 if way == 0 else -1
        arrive(tok_at(-sign * s, q), tok_sem(way, s, q))

    def dwn_rows(way, s):
        return (0, NEAR) if s < 4 else (NEAR // 2 * way, NEAR // 2)

    def dwn_step(way, s):
        sign = 1 if way == 0 else -1
        part = dwn_rows(way, s)
        send(
            dwn_at(-sign * (s - 1), 0, *part), dwn_at(-sign * s, 0, *part),
            along_y(sign), DY(way, s - 1),
        )

    def dwn_wait(way, s):
        sign = 1 if way == 0 else -1
        arrive(dwn_at(-sign * s, 0, *dwn_rows(way, s)), DY(way, s - 1))

    def dwn_piece(r, z):
        return dwn.at[cols((r % 8) * 256, NEAR), cols(z * 128, 128)]

    def far_at(r, way, s):
        first, n = (NEAR, 256 - NEAR) if s < 4 else (NEAR + (256 - NEAR) // 2 * way, (256 - NEAR) // 2)
        return dwn.at[cols((r % 8) * 256 + first, n), cols(0, 1024)]

    def far_step(way, s):
        sign = 1 if way == 0 else -1
        send(
            far_at(-sign * (s - 1), way, s), far_at(-sign * s, way, s), along_y(sign), EY(way, s - 1)
        )

    def far_wait(s):
        for way in range(2):
            sign = 1 if way == 0 else -1
            arrive(far_at(-sign * s, way, s), EY(way, s - 1))
            if s < 4:
                far_step(way, s + 1)

    def x_first(r):
        send(dwn_at(r, 0, 0, NEAR), dwn_at(r, 3, 0, NEAR), along_x(1), DX(0, r))
        send(dwn_at(r, 0, 0, NEAR), dwn_at(r, 1, 0, NEAR), along_x(-1), DX(1, r))

    def x_pieces(r):
        n = (256 if r == 0 else NEAR) // 2
        return (0, n), (n, n)

    def x_second(r):
        if r == 0:
            for way, rx in ((0, 3), (1, 1)):
                arrive(dwn.at[cols(0, 256), cols(rx * 256, 128)], D0(way))
                arrive(dwn.at[cols(0, 256), cols(rx * 256 + 128, 128)], DX(way, 0))
        else:
            arrive(dwn_at(r, 3, 0, NEAR), DX(0, r))
            arrive(dwn_at(r, 1, 0, NEAR), DX(1, r))
        low, high = x_pieces(r)
        send(dwn_at(r, 3, *low), dwn_at(r, 2, *low), along_x(1), DF(r))
        send(dwn_at(r, 1, *high), dwn_at(r, 2, *high), along_x(-1), DF(r))

    def core_half(r, rc):
        return dwn.at[cols((r % 8) * 256, 256), cols(rc * 1024, 1024)]

    def x_third(r):
        arrive(dwn_at(r, 2, 0, 256 if r == 0 else NEAR), DF(r))
        send(core_half(r, 0), core_half(r, 1), other_core, DC(r))

    def half_cols(way):
        return cols(way * 1024, 1024)

    def ring_z(ref, base, first):
        own, below, above, far = (ref.at[cols(base + 16 * k, 16)] for k in (0, 3, 1, 2))

        def start():
            send(own, below, along_z(1), first(0))
            send(own, above, along_z(-1), first(1))

        def forward():
            arrive(below, first(0))
            send(below.at[:, half_cols(0)], far.at[:, half_cols(0)], along_z(1), first(2))
            arrive(above, first(1))
            send(above.at[:, half_cols(1)], far.at[:, half_cols(1)], along_z(-1), first(2))

        def finish():
            arrive(far, first(2))

        return start, forward, finish

    tok_start, tok_forward, tok_finish = ring_z(tok, 0, TZ)
    got_down.wait()
    own_down = dwn.at[cols(0, 256), cols(0, 128)]
    send(own_down, dwn.at[cols(0, 256), cols(128, 128)], other_z, DZ(0))
    got_tok.wait()
    tok_start()
    for way in range(2):
        tok_step(way, 1, 0)
    for way, rx in ((0, 3), (1, 1)):
        send(own_down, dwn.at[cols(0, 256), cols(rx * 256, 128)], along_x(1 - 2 * way), D0(way))
        send(dwn_piece(0, 0), dwn_piece(2 * way - 1, 0), along_y(1 - 2 * way), DB(way))
    got_up.wait()
    send(up_own, up_own, other_z, UZ(0))
    got_p.wait()
    low, quarters = cols(0, 512), [cols(512 * k, 512) for k in range(1, 4)]

    def onward_part(k):
        return message(pbuf.at[quarters[k]], prel.at[cols(512 * k, 512)], onward, PR(k), ON_SENT)

    def corner_part(k):
        return message(prel.at[cols(512 * k, 512)], pof.at[quarters[k]], corner, PO(1 + k), ON_SENT)

    def straight_part(k):
        return message(pbuf.at[quarters[k]], pof.at[quarters[k]], off_chip, PO(1 + k), STRAIGHT_SENT)

    direct_part = message(pbuf.at[low], pof.at[low], off_chip, PO(0), BLOCK_SENT)

    @pl.when(diagonal)
    def _():
        onward_part(0).start()

    send(pbuf, pin, other_core, PI(0))
    got_t.wait()
    send(tbuf, tin, other_core, TI(0))

    z_down = dwn.at[cols(0, 256), cols(128, 128)]
    arrive(z_down, DZ(0))
    for way, rx in ((0, 3), (1, 1)):
        send(dwn_piece(0, 1), dwn_piece(2 * way - 1, 1), along_y(1 - 2 * way), DY(way, 0))
        send(z_down, dwn.at[cols(0, 256), cols(rx * 256 + 128, 128)], along_x(1 - 2 * way), DX(way, 0))
    tok_forward()
    for way in range(2):
        tok_step(way, 1, 3)
        tok_step(way, 1, 1)

    @pl.when(diagonal)
    def _():
        onward_part(1).start()

    arrive(upb.at[x, 1 - zl, c], UZ(0))
    send(upb.at[x, :, c], upb.at[x, :, c], along_x(1), UX(0))
    send(upb.at[x, :, c], upb.at[x, :, c], along_x(-1), UX(1))

    @pl.when(jnp.logical_not(diagonal))
    def _():
        direct_part.start()
        for k in range(3):
            straight_part(k).start()

    tok_finish()
    for way in range(2):
        tok_step(way, 1, 2)
    pltpu.make_async_copy(tgt, tgt, lsem.at[5]).wait()

    def down(s):
        for way in range(2):
            if s == 1:
                arrive(dwn_piece(2 * way - 1, 0), DB(way))
                arrive(dwn_piece(2 * way - 1, 1), DY(way, 0))
            else:
                dwn_wait(way, s)
            if s < 4:
                dwn_step(way, s + 1)
        if s == 1:
            x_second(0)
        for r in (8 - s, s)[: 2 if s < 4 else 1]:
            x_first(r)

    def token(s, *pieces):
        for q in pieces:
            for way in range(2):
                if s <= tok_steps(way, q):
                    tok_wait(way, s, q)
                    if s < tok_steps(way, q):
                        tok_step(way, s + 1, q)

    down(1)
    token(1, 0, 3)
    down(2)
    whole_t = message(tbuf, tof, off_chip, TO(0), BLOCK_SENT)

    @pl.when(jnp.logical_not(diagonal))
    def _():
        whole_t.start()

    def track_piece(k):
        rows = cols(1024 * k, 1024)

        @pl.when(diagonal)
        def _():
            message(tbuf.at[rows], tof.at[rows], off_chip, TO(0), BLOCK_SENT).start()

    below, above, across = (x + 3) % 4, (x + 1) % 4, (x + 2) % 4
    arrive(upb.at[below, :, c], UX(0))
    send(upb.at[below, 0, c], upb.at[below, 0, c], along_x(1), UF(0))
    arrive(upb.at[above, :, c], UX(1))
    send(upb.at[above, 1, c], upb.at[above, 1, c], along_x(-1), UF(0))
    token(1, 1, 2)

    @pl.when(diagonal)
    def _():
        onward_part(2).start()
        for k in range(2):
            arrive(prel.at[cols(512 * k, 512)], PR(k))
            corner_part(k).start()

    token(2, 0)
    x_third(0)
    for way in range(2):
        far_step(way, 1)
    down(3)

    @pl.when(diagonal)
    def _():
        direct_part.start()

    token(2, 3, 1)
    x_second(7)
    x_second(1)
    down(4)
    token(2, 2)
    far_wait(1)

    @pl.when(diagonal)
    def _():
        arrive(prel.at[cols(1024, 512)], PR(2))
        corner_part(2).start()

    token(3, 0, 3)
    x_second(6)
    x_second(2)
    arrive(upb.at[across, :, c], UF(0))
    send(upb.at[:, :, c], upb.at[:, :, c], other_core, UC(0))
    token(3, 1, 2)
    far_wait(2)
    x_third(7)
    x_third(1)
    token(4, 0, 3, 1, 2)
    far_wait(3)

    def rows256(i):
        return pl.ds(pl.multiple_of(i * 256, 256), 256)

    arrive(upb.at[:, :, 1 - c], UC(0))

    def hidden_half(p, weights, half):
        rows = cols(256 * half, 256)
        if p == 0:
            sums = jnp.zeros((256, 256), F32)
            for k in range(8):
                sums += jnp.dot(
                    tok[rows, k * 256 : (k + 1) * 256],
                    upb[k // 2, k % 2].reshape(256, 256),
                    preferred_element_type=F32,
                )
            upv[rows, :] = sums
        gate = jnp.dot(tok[rows, :], weights[...], preferred_element_type=F32) * scale
        sig = jax.nn.sigmoid(gate)
        up = upv[rows, :]
        hsend[p, rows, :] = (sig * gate * up).astype(BF16)
        fac[p, rows, :] = up * sig * (1.0 + gate * (1.0 - sig))

    def hidden_of(p, weights):
        for half, blocks in ((1, (4, 5, 6, 7)), (0, (3, 2, 1))):
            hidden_half(p, weights, half)
            for r in blocks:
                send(
                    hsend.at[p, cols(r * 64, 64)], hall.at[p, :, cols((8 - r) * 256, 256)],
                    along_y(r), HI(p),
                )
        hall[p, :, 0:256] = hsend[p, 0:64, :]

    hidden_of(0, pbuf)
    x_second(5)
    x_second(3)
    x_second(4)

    e_off = edge[(a + c + 15) % 16]
    e_in = edge[(a + 16 - c) % 16]
    own = 1.0 - e_off - e_in
    eta = step[0]
    arrive(pin, PI(0))
    arrive(pof.at[low], PO(0))
    for k in range(3):
        arrive(pof.at[quarters[k]], PO(1 + k))

    @pl.loop(0, 8)
    def _(i):
        rows = rows256(i)
        mixed = own * pbuf[rows, :].astype(F32)
        mixed += e_off * pof[rows, :].astype(F32) + e_in * pin[rows, :].astype(F32)
        fresh[rows, :] = (mixed - eta * tbuf[rows, :].astype(F32)).astype(BF16)

    fresh_copy = pltpu.make_async_copy(fresh, fresh_out.at[0], lsem.at[6])
    fresh_copy.start()
    hidden_of(1, fresh)
    track_piece(0)
    x_third(6)
    x_third(2)
    far_wait(4)
    x_third(5)
    x_third(3)
    x_third(4)

    def sum_first(p, way):
        rows, part = cols(32, 16), half_cols(way)
        return psend.at[p, rows, part], pmid.at[p, :, part]

    def sum_second(p, way, half):
        rows, part = cols(16 + 32 * way, 16), half_cols(half)
        return psend.at[p, rows, part], prec.at[p, way, :, part]

    def hidden_wait(p):
        arrive(hall.at[p, :, cols(256, 1792)], HI(p))

    def partial_of(p):
        hidden_wait(p)
        for half in range(2):
            if p == 0 and half == 1:
                for r in ORDER:
                    arrive(core_half(r, 1), DC(r))

            @pl.loop(4 * half, 4 * half + 4)
            def _(i):
                part = jnp.dot(hall[p], dwn[:, rows256(i)], preferred_element_type=F32)
                psend[p, :, rows256(i)] = part.astype(BF16)

            send(*sum_first(p, half), along_z(1 - 2 * half), RS(p, half))
            send(*sum_second(p, 1 - half, half), along_z(2 * half - 1), RS(p, 2))

    def middle_of(p):
        for way in range(2):
            arrive(sum_first(p, way)[1], RS(p, way))
            rows, part = cols(16 + 32 * way, 16), half_cols(way)
            both = psend[p, rows, part].astype(F32) + pmid[p, :, part].astype(F32)
            psend[p, rows, part] = both.astype(BF16)
            send(*sum_second(p, way, way), along_z(1 - 2 * way), RS(p, 2))

    err_ring = [ring_z(eall.at[p], 0, functools.partial(EG, p)) for p in range(2)]

    def err_of(p):
        out = psend[p, 0:16, :].astype(F32)
        arrive(prec.at[p], RS(p, 2))
        for way in range(2):
            out += prec[p, way].astype(F32)
        eall[p, 0:16, :] = (2.0 * (out - tgt[...].astype(F32))).astype(BF16)
        err_ring[p][0]()

    partial_of(0)
    partial_of(1)
    middle_of(0)
    middle_of(1)
    err_of(0)
    err_of(1)
    for p in range(2):
        err_ring[p][1]()
    track_piece(1)

    def back_block(p, r):
        return lax.dot_general(
            eall[p], dwn[pl.ds(pl.multiple_of(r * 256, 256), 256), :],
            (((1,), (1,)), ((), ())), preferred_element_type=F32,
        ).astype(BF16)

    def back_message(p, r):
        rows = pl.ds(pl.multiple_of(r * 64, 64), 64)
        land = pl.ds(pl.multiple_of((8 - r) * 64, 64), 64)
        return message(bsend.at[p, rows], brec.at[p, land], along_y(r), BK(p), BACK_SENT)

    def back_of(p):
        err_ring[p][2]()

        @pl.loop(0, 7)
        def _(k):
            r = 4 + ((k + 1) // 2) * (1 - 2 * (k % 2))
            bsend[p, pl.ds(pl.multiple_of(r * 64, 64), 64), :] = back_block(p, r)
            back_message(p, r).start()

        brec[p, 0:64, :] = back_block(p, 0)

    back_of(0)
    back_of(1)

    arrive(tin, TI(0))
    arrive(tof, TO(0))

    def prepare():
        @pl.loop(0, 8)
        def _(i):
            rows = rows256(i)
            turned[rows, :] = tok[:, rows].T
            mixed = own * tbuf[rows, :].astype(F32)
            mixed += e_off * tof[rows, :].astype(F32) + e_in * tin[rows, :].astype(F32)
            mixed_y[rows, :] = mixed

    prepare()
    turned_copy = pltpu.make_async_copy(turned, turned_out, lsem.at[7])
    mixed_copy = pltpu.make_async_copy(mixed_y, mixed_out, lsem.at[0])
    turned_copy.start()
    mixed_copy.start()

    for p in range(2):
        arrive(brec.at[p, cols(64, 448)], BK(p))

    dd[...] = (
        brec[1].astype(F32) * fac[1] - brec[0].astype(F32) * fac[0]
    ).astype(BF16)

    dd_copy = pltpu.make_async_copy(dd, dd_out, lsem.at[5])
    dd_copy.start()

    for g, nbytes in enumerate(sent):
        if nbytes:
            all_sent(nbytes, g)
    all_sent(5 << 18, BLOCK_SENT)
    all_sent(14 << 15, BACK_SENT)

    @pl.when(diagonal)
    def _():
        all_sent(3 << 19, ON_SENT)

    @pl.when(jnp.logical_not(diagonal))
    def _():
        all_sent(3 << 18, STRAIGHT_SENT)

    fresh_copy.wait()
    turned_copy.wait()
    mixed_copy.wait()
    dd_copy.wait()


def last_kernel(
    dd_in, turned_in, mixed_in, fresh_in, fresh_out, track_out,
    dd, turned, mixed, fresh, track, sem, out_sem,
):
    first = pltpu.make_async_copy(dd_in, dd, sem.at[0])
    first.start()
    pieces = []
    for k in range(PARTS):
        rows = pl.ds(k * (2048 // PARTS), 2048 // PARTS)
        a = pltpu.make_async_copy(turned_in.at[rows], turned.at[rows], sem.at[1 + 2 * k])
        b = pltpu.make_async_copy(mixed_in.at[rows], mixed.at[rows], sem.at[2 + 2 * k])
        a.start()
        b.start()
        pieces.append((rows, a, b))
    middle = pltpu.make_async_copy(fresh_in, fresh, sem.at[1 + 2 * PARTS])
    middle.start()
    done = []
    first.wait()
    for k, (rows, a, b) in enumerate(pieces):
        a.wait()
        b.wait()
        change = jnp.dot(turned[rows, :], dd[...], preferred_element_type=F32)
        track[rows, :] = (mixed[rows, :] + change * 2048.0 ** -0.5).astype(BF16)
        done.append(pltpu.make_async_copy(track.at[rows], track_out.at[0, rows], out_sem.at[k]))
        done[-1].start()
        if k == PARTS - 2:
            middle.wait()
            done.append(pltpu.make_async_copy(fresh, fresh_out, out_sem.at[PARTS]))
            done[-1].start()
    for copy in done:
        copy.wait()


def on_device(tokens, targets, params, tracker, up_weight, down_weight, edge_weight, step_size):
    hbm = pl.BlockSpec(memory_space=pltpu.HBM)
    smem = pl.BlockSpec(memory_space=pltpu.SMEM)
    block = pltpu.VMEM((2048, 256), BF16)
    out = jax.ShapeDtypeStruct(params.shape, BF16)
    fresh, dd, turned, mixed = pl.pallas_call(
        kernel,
        out_shape=(
            out,
            jax.ShapeDtypeStruct((512, 256), BF16),
            jax.ShapeDtypeStruct((2048, 512), BF16),
            jax.ShapeDtypeStruct((2048, 256), F32),
        ),
        in_specs=[smem, smem] + [hbm] * 6,
        out_specs=(hbm, hbm, hbm, hbm),
        scratch_shapes=[
            pltpu.VMEM((512, 2048), BF16),
            pltpu.VMEM((16, 2048), BF16),
            block, block, block, block, block, block, block,
            pltpu.VMEM((4, 2, 2, 128, 256), BF16),
            pltpu.VMEM((2048, 2048), BF16),
            pltpu.VMEM((512, 256), F32),
            pltpu.VMEM((2, 512, 256), F32),
            pltpu.VMEM((2, 512, 256), BF16),
            pltpu.VMEM((2, 64, 2048), BF16),
            pltpu.VMEM((2, 64, 2048), BF16),
            pltpu.VMEM((2, 16, 2048), BF16),
            pltpu.VMEM((2, 2, 16, 2048), BF16),
            pltpu.VMEM((2, 64, 2048), BF16),
            pltpu.VMEM((2, 512, 256), BF16),
            pltpu.VMEM((2, 512, 256), BF16),
            pltpu.VMEM((512, 256), BF16),
            pltpu.VMEM((1536, 256), BF16),
            pltpu.VMEM((2048, 512), BF16),
            pltpu.VMEM((2048, 256), F32),
            pltpu.SemaphoreType.DMA((SENDS + 4,)),
            pltpu.SemaphoreType.DMA((SEMS,)),
            pltpu.SemaphoreType.DMA((8,)),
        ],
        compiler_params=pltpu.CompilerParams(
            collective_id=0, has_side_effects=True, vmem_limit_bytes=56 * 1024 * 1024
        ),
    )(edge_weight, step_size, tokens, targets, params, tracker, up_weight, down_weight)
    return pl.pallas_call(
        last_kernel,
        out_shape=(out, out),
        in_specs=[hbm] * 4,
        out_specs=(hbm, hbm),
        scratch_shapes=[
            pltpu.VMEM((512, 256), BF16),
            pltpu.VMEM((2048, 512), BF16),
            pltpu.VMEM((2048, 256), F32),
            pltpu.VMEM((1, 2048, 256), BF16),
            block,
            pltpu.SemaphoreType.DMA((2 + 2 * PARTS,)),
            pltpu.SemaphoreType.DMA((1 + PARTS,)),
        ],
    )(dd, turned, mixed, fresh)


def solution(mesh):
    in_specs = (
        P("agent", "tp", None),
        P("agent", "tp", None),
        P("agent", None, "tp"),
        P("agent", None, "tp"),
        P("agent", "tp"),
        P("tp", "agent"),
        P(),
        P(),
    )
    out_specs = (P("agent", None, "tp"), P("agent", None, "tp"))
    return jax.shard_map(
        on_device, mesh=mesh, in_specs=in_specs, out_specs=out_specs, check_vma=False
    )
```

```python
import functools
import math

import jax
import jax.numpy as jnp
from jax import lax
from jax.experimental import pallas as pl
from jax.experimental.pallas import tpu as pltpu
from jax.sharding import PartitionSpec as P

MESH = pl.DeviceIdType.MESH
BF16 = jnp.bfloat16
F32 = jnp.float32
ORDER = (0, 7, 1, 6, 2, 5, 3, 4)
NEAR = 224
PARTS = 4
FAR_FIRST = (4, 3, 5, 2, 6, 1, 7)


class Plan:
    def __init__(self):
        self.count = 0

    def take(self, *shape):
        size = 1
        for n in shape:
            size *= n
        base = self.count
        self.count += size

        def number(*index):
            flat = 0
            for i, n in zip(index, shape):
                flat = flat * n + i
            return base + flat

        return number


plan = Plan()
TZ, TY = plan.take(3), plan.take(2, 2, 7)
UZ, UX, UF, UC = plan.take(1), plan.take(2), plan.take(1), plan.take(1)
DZ, DB, D0 = plan.take(1), plan.take(2), plan.take(2)
DY, EY = plan.take(2, 4), plan.take(2, 4)
DX, DF, DC = plan.take(2, 8), plan.take(8), plan.take(8)
PI, PO, TI, TO, PR = plan.take(1), plan.take(4), plan.take(1), plan.take(1), plan.take(3)
HI, BK = plan.take(2), plan.take(2)
RS, EG = plan.take(2, 3), plan.take(2, 3)
SEMS = plan.count
SENDS = 8
BLOCK_SENT, ON_SENT, STRAIGHT_SENT, BACK_SENT = range(SENDS, SENDS + 4)

def kernel(
    edge, step, tokens, targets, params, tracker, up_w, down_w, fresh_out, dd_out, turned_out, mixed_out,
    tok, tgt, pbuf, tbuf, pin, pof, tin, tof, fresh, upb, dwn, upv, fac, hsend, hall,
    psend, pmid, prec, eall, bsend, brec, dd, prel, turned, mixed_y, ssem, rsem, lsem,
):
    a = lax.axis_index("agent")
    t = lax.axis_index("tp")
    x, zl, c = a // 4, (a // 2) % 2, a % 2
    zh, y = t // 8, t % 8
    scale = 2048.0 ** -0.5

    def along_y(r):
        return (a, zh * 8 + (y + r + 8) % 8)

    def along_z(q):
        return (a, ((zh + q + 4) % 4) * 8 + y)

    def along_x(r):
        return ((a + 4 * r + 16) % 16, t)

    other_core = (a + 1 - 2 * c, t)
    off_chip = ((a + 2 * c + 15) % 16, t)
    other_z = (a + 2 - 4 * zl, t)
    onward = ((a + 8 * c + 12) % 16, t)
    corner = (4 * x + 3 - (a % 4), t)
    diagonal = c == zl

    def cols(first, n):
        return pl.ds(first, n)

    barrier = pltpu.get_barrier_semaphore()
    peers = [other_core, off_chip, other_z, corner, along_x(1), along_x(-1)]
    peers += [along_y(r) for r in range(1, 8)] + [along_z(1), along_z(-1)]
    for peer in peers:
        pl.semaphore_signal(barrier, inc=1, device_id=peer, device_id_type=MESH)

    def fetch(src, dst, k):
        copy = pltpu.make_async_copy(src, dst, lsem.at[k])
        copy.start()
        return copy

    up_own = upb.at[x, zl, c]
    got_tok = fetch(tokens.at[0], tok.at[cols(0, 16)], 0)
    got_up = fetch(up_w, up_own, 1)
    got_down = fetch(down_w, dwn.at[cols(0, 256), cols(0, 128)], 2)
    got_p = fetch(params.at[0], pbuf, 3)
    got_t = fetch(tracker.at[0], tbuf, 4)
    for rc in range(2):
        for rx in range(4):
            for rz in range(2):
                who = ((x + rx) % 4) * 4 + ((zl + rz) % 2) * 2 + (c + rc) % 2
                src = targets.at[0, :, pl.ds(pl.multiple_of(who * 128, 128), 128)]
                fetch(src, tgt.at[:, cols(rc * 1024 + rx * 256 + rz * 128, 128)], 5)

    pl.semaphore_wait(barrier, len(peers))

    sent = [0]

    def message(src, dst, peer, k, out=0):
        return pltpu.make_async_remote_copy(
            src_ref=src, dst_ref=dst, send_sem=ssem.at[out], recv_sem=rsem.at[k],
            device_id=peer, device_id_type=MESH,
        )

    def send(src, dst, peer, k):
        message(src, dst, peer, k, len(sent) - 1).start()
        sent[-1] += math.prod(src.shape) * 2
        if sent[-1] >= 5 << 19 and sent[-1] % (1 << 15) == 0:
            sent.append(0)

    def arrive(dst, k):
        message(dst, dst, other_core, k).wait_recv()

    def all_sent(nbytes, out):
        rows = dwn.at[cols(0, nbytes // 2048), cols(0, 1024)]
        message(rows, rows, other_core, 0, out).wait_send()

    def tok_at(r, q):
        return tok.at[cols((r % 8) * 64 + (q % 4) * 16, 16)]

    def dwn_at(r, rx, first=0, rows=256):
        return dwn.at[cols((r % 8) * 256 + first, rows), cols(rx * 256, 256)]

    def tok_steps(way, q):
        return 4 if (q < 2) == (way == 0) else 3

    def tok_sem(way, s, q):
        pair, rank = divmod(q, 2)
        if pair == way:
            return TY(way, rank, s - 1)
        return TY(way, rank, 3 + s)

    def tok_step(way, s, q):
        sign = 1 if way == 0 else -1
        send(tok_at(-sign * (s - 1), q), tok_at(-sign * s, q), along_y(sign), tok_sem(way, s, q))

    def tok_wait(way, s, q):
        sign = 1 if way == 0 else -1
        arrive(tok_at(-sign * s, q), tok_sem(way, s, q))

    def dwn_rows(way, s):
        return (0, NEAR) if s < 4 else (NEAR // 2 * way, NEAR // 2)

    def dwn_step(way, s):
        sign = 1 if way == 0 else -1
        part = dwn_rows(way, s)
        send(
            dwn_at(-sign * (s - 1), 0, *part), dwn_at(-sign * s, 0, *part),
            along_y(sign), DY(way, s - 1),
        )

    def dwn_wait(way, s):
        sign = 1 if way == 0 else -1
        arrive(dwn_at(-sign * s, 0, *dwn_rows(way, s)), DY(way, s - 1))

    def dwn_piece(r, z):
        return dwn.at[cols((r % 8) * 256, NEAR), cols(z * 128, 128)]

    def far_at(r, way, s):
        first, n = (NEAR, 256 - NEAR) if s < 4 else (NEAR + (256 - NEAR) // 2 * way, (256 - NEAR) // 2)
        return dwn.at[cols((r % 8) * 256 + first, n), cols(0, 1024)]

    def far_step(way, s):
        sign = 1 if way == 0 else -1
        send(
            far_at(-sign * (s - 1), way, s), far_at(-sign * s, way, s), along_y(sign), EY(way, s - 1)
        )

    def far_wait(s):
        for way in range(2):
            sign = 1 if way == 0 else -1
            arrive(far_at(-sign * s, way, s), EY(way, s - 1))
            if s < 4:
                far_step(way, s + 1)

    def x_first(r):
        send(dwn_at(r, 0, 0, NEAR), dwn_at(r, 3, 0, NEAR), along_x(1), DX(0, r))
        send(dwn_at(r, 0, 0, NEAR), dwn_at(r, 1, 0, NEAR), along_x(-1), DX(1, r))

    def x_pieces(r):
        n = (256 if r == 0 else NEAR) // 2
        return (0, n), (n, n)

    def x_second(r):
        if r == 0:
            for way, rx in ((0, 3), (1, 1)):
                arrive(dwn.at[cols(0, 256), cols(rx * 256, 128)], D0(way))
                arrive(dwn.at[cols(0, 256), cols(rx * 256 + 128, 128)], DX(way, 0))
        else:
            arrive(dwn_at(r, 3, 0, NEAR), DX(0, r))
            arrive(dwn_at(r, 1, 0, NEAR), DX(1, r))
        low, high = x_pieces(r)
        send(dwn_at(r, 3, *low), dwn_at(r, 2, *low), along_x(1), DF(r))
        send(dwn_at(r, 1, *high), dwn_at(r, 2, *high), along_x(-1), DF(r))

    def core_half(r, rc):
        return dwn.at[cols((r % 8) * 256, 256), cols(rc * 1024, 1024)]

    def x_third(r):
        arrive(dwn_at(r, 2, 0, 256 if r == 0 else NEAR), DF(r))
        send(core_half(r, 0), core_half(r, 1), other_core, DC(r))

    def half_cols(way):
        return cols(way * 1024, 1024)

    def ring_z(ref, base, first):
        own, below, above, far = (ref.at[cols(base + 16 * k, 16)] for k in (0, 3, 1, 2))

        def start():
            send(own, below, along_z(1), first(0))
            send(own, above, along_z(-1), first(1))

        def forward():
            arrive(below, first(0))
            send(below.at[:, half_cols(0)], far.at[:, half_cols(0)], along_z(1), first(2))
            arrive(above, first(1))
            send(above.at[:, half_cols(1)], far.at[:, half_cols(1)], along_z(-1), first(2))

        def finish():
            arrive(far, first(2))

        return start, forward, finish

    tok_start, tok_forward, tok_finish = ring_z(tok, 0, TZ)
    got_down.wait()
    own_down = dwn.at[cols(0, 256), cols(0, 128)]
    send(own_down, dwn.at[cols(0, 256), cols(128, 128)], other_z, DZ(0))
    got_tok.wait()
    tok_start()
    for way in range(2):
        tok_step(way, 1, 0)
    for way, rx in ((0, 3), (1, 1)):
        send(own_down, dwn.at[cols(0, 256), cols(rx * 256, 128)], along_x(1 - 2 * way), D0(way))
        send(dwn_piece(0, 0), dwn_piece(2 * way - 1, 0), along_y(1 - 2 * way), DB(way))
    got_up.wait()
    send(up_own, up_own, other_z, UZ(0))
    got_p.wait()
    low, quarters = cols(0, 512), [cols(512 * k, 512) for k in range(1, 4)]

    def onward_part(k):
        return message(pbuf.at[quarters[k]], prel.at[cols(512 * k, 512)], onward, PR(k), ON_SENT)

    def corner_part(k):
        return message(prel.at[cols(512 * k, 512)], pof.at[quarters[k]], corner, PO(1 + k), ON_SENT)

    def straight_part(k):
        return message(pbuf.at[quarters[k]], pof.at[quarters[k]], off_chip, PO(1 + k), STRAIGHT_SENT)

    direct_part = message(pbuf.at[low], pof.at[low], off_chip, PO(0), BLOCK_SENT)

    @pl.when(diagonal)
    def _():
        onward_part(0).start()

    send(pbuf, pin, other_core, PI(0))
    got_t.wait()
    send(tbuf, tin, other_core, TI(0))

    z_down = dwn.at[cols(0, 256), cols(128, 128)]
    arrive(z_down, DZ(0))
    for way, rx in ((0, 3), (1, 1)):
        send(dwn_piece(0, 1), dwn_piece(2 * way - 1, 1), along_y(1 - 2 * way), DY(way, 0))
        send(z_down, dwn.at[cols(0, 256), cols(rx * 256 + 128, 128)], along_x(1 - 2 * way), DX(way, 0))
    tok_forward()
    for way in range(2):
        tok_step(way, 1, 3)
        tok_step(way, 1, 1)

    @pl.when(diagonal)
    def _():
        onward_part(1).start()

    arrive(upb.at[x, 1 - zl, c], UZ(0))
    send(upb.at[x, :, c], upb.at[x, :, c], along_x(1), UX(0))
    send(upb.at[x, :, c], upb.at[x, :, c], along_x(-1), UX(1))

    @pl.when(jnp.logical_not(diagonal))
    def _():
        direct_part.start()
        for k in range(3):
            straight_part(k).start()

    tok_finish()
    for way in range(2):
        tok_step(way, 1, 2)
    pltpu.make_async_copy(tgt, tgt, lsem.at[5]).wait()

    def down(s):
        for way in range(2):
            if s == 1:
                arrive(dwn_piece(2 * way - 1, 0), DB(way))
                arrive(dwn_piece(2 * way - 1, 1), DY(way, 0))
            else:
                dwn_wait(way, s)
            if s < 4:
                dwn_step(way, s + 1)
        if s == 1:
            x_second(0)
        for r in (8 - s, s)[: 2 if s < 4 else 1]:
            x_first(r)

    def token(s, *pieces):
        for q in pieces:
            for way in range(2):
                if s <= tok_steps(way, q):
                    tok_wait(way, s, q)
                    if s < tok_steps(way, q):
                        tok_step(way, s + 1, q)

    down(1)
    token(1, 0, 3)
    down(2)
    whole_t = message(tbuf, tof, off_chip, TO(0), BLOCK_SENT)

    @pl.when(jnp.logical_not(diagonal))
    def _():
        whole_t.start()

    below, above, across = (x + 3) % 4, (x + 1) % 4, (x + 2) % 4
    arrive(upb.at[below, :, c], UX(0))
    send(upb.at[below, 0, c], upb.at[below, 0, c], along_x(1), UF(0))
    arrive(upb.at[above, :, c], UX(1))
    send(upb.at[above, 1, c], upb.at[above, 1, c], along_x(-1), UF(0))
    token(1, 1, 2)

    @pl.when(diagonal)
    def _():
        onward_part(2).start()
        for k in range(2):
            arrive(prel.at[cols(512 * k, 512)], PR(k))
            corner_part(k).start()

    token(2, 0)
    x_third(0)
    for way in range(2):
        far_step(way, 1)
    down(3)

    @pl.when(diagonal)
    def _():
        direct_part.start()

    token(2, 3, 1)
    x_second(7)
    x_second(1)
    down(4)
    token(2, 2)
    far_wait(1)

    token(3, 0, 3)
    x_second(6)
    x_second(2)
    arrive(upb.at[across, :, c], UF(0))
    send(upb.at[:, :, c], upb.at[:, :, c], other_core, UC(0))
    token(3, 1, 2)
    far_wait(2)
    x_third(7)
    x_third(1)

    @pl.when(diagonal)
    def _():
        arrive(prel.at[cols(1024, 512)], PR(2))
        corner_part(2).start()

    token(4, 0, 3, 1, 2)
    far_wait(3)

    def rows256(i):
        return pl.ds(pl.multiple_of(i * 256, 256), 256)

    arrive(upb.at[:, :, 1 - c], UC(0))

    def hidden_half(p, weights, half):
        rows = cols(256 * half, 256)
        if p == 0:
            sums = jnp.zeros((256, 256), F32)
            for k in range(8):
                sums += jnp.dot(
                    tok[rows, k * 256 : (k + 1) * 256],
                    upb[k // 2, k % 2].reshape(256, 256),
                    preferred_element_type=F32,
                )
            upv[rows, :] = sums
        gate = jnp.dot(tok[rows, :], weights[...], preferred_element_type=F32) * scale
        sig = jax.nn.sigmoid(gate)
        up = upv[rows, :]
        hsend[p, rows, :] = (sig * gate * up).astype(BF16)
        fac[p, rows, :] = up * sig * (1.0 + gate * (1.0 - sig))

    def hidden_of(p, weights):
        for half, blocks in ((1, (4, 5, 6, 7)), (0, (3, 2, 1))):
            hidden_half(p, weights, half)
            for r in blocks:
                send(
                    hsend.at[p, cols(r * 64, 64)], hall.at[p, :, cols((8 - r) * 256, 256)],
                    along_y(r), HI(p),
                )
        hall[p, :, 0:256] = hsend[p, 0:64, :]

    hidden_of(0, pbuf)
    x_second(5)
    x_second(3)
    x_second(4)

    e_off = edge[(a + c + 15) % 16]
    e_in = edge[(a + 16 - c) % 16]
    own = 1.0 - e_off - e_in
    eta = step[0]
    arrive(pin, PI(0))
    arrive(pof.at[low], PO(0))
    for k in range(3):
        arrive(pof.at[quarters[k]], PO(1 + k))

    @pl.loop(0, 8)
    def _(i):
        rows = rows256(i)
        mixed = own * pbuf[rows, :].astype(F32)
        mixed += e_off * pof[rows, :].astype(F32) + e_in * pin[rows, :].astype(F32)
        fresh[rows, :] = (mixed - eta * tbuf[rows, :].astype(F32)).astype(BF16)

    fresh_copy = pltpu.make_async_copy(fresh, fresh_out.at[0], lsem.at[6])
    fresh_copy.start()
    hidden_of(1, fresh)
    x_third(6)
    x_third(2)
    far_wait(4)
    x_third(5)
    x_third(3)
    x_third(4)

    def sum_first(p, way):
        rows, part = cols(32, 16), half_cols(way)
        return psend.at[p, rows, part], pmid.at[p, :, part]

    def sum_second(p, way, half):
        rows, part = cols(16 + 32 * way, 16), half_cols(half)
        return psend.at[p, rows, part], prec.at[p, way, :, part]

    def hidden_wait(p):
        arrive(hall.at[p, :, cols(256, 1792)], HI(p))

    def partial_of(p):
        hidden_wait(p)
        for half in range(2):
            if p == 0 and half == 1:
                for r in ORDER:
                    arrive(core_half(r, 1), DC(r))

            @pl.loop(4 * half, 4 * half + 4)
            def _(i):
                part = jnp.dot(hall[p], dwn[:, rows256(i)], preferred_element_type=F32)
                psend[p, :, rows256(i)] = part.astype(BF16)

            send(*sum_first(p, half), along_z(1 - 2 * half), RS(p, half))
            send(*sum_second(p, 1 - half, half), along_z(2 * half - 1), RS(p, 2))

    def middle_of(p):
        for way in range(2):
            arrive(sum_first(p, way)[1], RS(p, way))
            rows, part = cols(16 + 32 * way, 16), half_cols(way)
            both = psend[p, rows, part].astype(F32) + pmid[p, :, part].astype(F32)
            psend[p, rows, part] = both.astype(BF16)
            send(*sum_second(p, way, way), along_z(1 - 2 * way), RS(p, 2))

    err_ring = [ring_z(eall.at[p], 0, functools.partial(EG, p)) for p in range(2)]

    def err_of(p):
        out = psend[p, 0:16, :].astype(F32)
        arrive(prec.at[p], RS(p, 2))
        for way in range(2):
            out += prec[p, way].astype(F32)
        eall[p, 0:16, :] = (2.0 * (out - tgt[...].astype(F32))).astype(BF16)
        err_ring[p][0]()

    partial_of(0)
    partial_of(1)
    middle_of(0)
    middle_of(1)
    err_of(0)
    err_of(1)
    for p in range(2):
        err_ring[p][1]()

    @pl.when(diagonal)
    def _():
        whole_t.start()


    def back_block(p, r):
        return lax.dot_general(
            eall[p], dwn[pl.ds(pl.multiple_of(r * 256, 256), 256), :],
            (((1,), (1,)), ((), ())), preferred_element_type=F32,
        ).astype(BF16)

    def back_message(p, r):
        rows = pl.ds(pl.multiple_of(r * 64, 64), 64)
        land = pl.ds(pl.multiple_of((8 - r) * 64, 64), 64)
        return message(bsend.at[p, rows], brec.at[p, land], along_y(r), BK(p), BACK_SENT)

    def back_of(p):
        err_ring[p][2]()

        @pl.loop(0, 7)
        def _(k):
            r = 4 + ((k + 1) // 2) * (1 - 2 * (k % 2))
            bsend[p, pl.ds(pl.multiple_of(r * 64, 64), 64), :] = back_block(p, r)
            back_message(p, r).start()

        brec[p, 0:64, :] = back_block(p, 0)

    back_of(0)
    back_of(1)

    def turn():
        @pl.loop(0, 8)
        def _(i):
            rows = rows256(i)
            turned[rows, :] = tok[:, rows].T

    def prepare():
        @pl.loop(0, 8)
        def _(i):
            rows = rows256(i)
            mixed = own * tbuf[rows, :].astype(F32)
            mixed += e_off * tof[rows, :].astype(F32) + e_in * tin[rows, :].astype(F32)
            mixed_y[rows, :] = mixed

    turn()
    arrive(tin, TI(0))
    arrive(tof, TO(0))
    prepare()
    turned_copy = pltpu.make_async_copy(turned, turned_out, lsem.at[7])
    mixed_copy = pltpu.make_async_copy(mixed_y, mixed_out, lsem.at[0])
    turned_copy.start()
    mixed_copy.start()

    for p in range(2):
        arrive(brec.at[p, cols(64, 448)], BK(p))

    dd[...] = (
        brec[1].astype(F32) * fac[1] - brec[0].astype(F32) * fac[0]
    ).astype(BF16)

    dd_copy = pltpu.make_async_copy(dd, dd_out, lsem.at[5])
    dd_copy.start()

    for g, nbytes in enumerate(sent):
        if nbytes:
            all_sent(nbytes, g)
    all_sent(5 << 18, BLOCK_SENT)
    all_sent(14 << 15, BACK_SENT)

    @pl.when(diagonal)
    def _():
        all_sent(3 << 19, ON_SENT)

    @pl.when(jnp.logical_not(diagonal))
    def _():
        all_sent(3 << 18, STRAIGHT_SENT)

    fresh_copy.wait()
    turned_copy.wait()
    mixed_copy.wait()
    dd_copy.wait()


def last_kernel(
    dd_in, turned_in, mixed_in, fresh_in, fresh_out, track_out,
    dd, turned, mixed, fresh, track, sem, out_sem,
):
    first = pltpu.make_async_copy(dd_in, dd, sem.at[0])
    first.start()
    pieces = []
    for k in range(PARTS):
        rows = pl.ds(k * (2048 // PARTS), 2048 // PARTS)
        a = pltpu.make_async_copy(turned_in.at[rows], turned.at[rows], sem.at[1 + 2 * k])
        b = pltpu.make_async_copy(mixed_in.at[rows], mixed.at[rows], sem.at[2 + 2 * k])
        a.start()
        b.start()
        pieces.append((rows, a, b))
    middle = pltpu.make_async_copy(fresh_in, fresh, sem.at[1 + 2 * PARTS])
    middle.start()
    done = []
    first.wait()
    for k, (rows, a, b) in enumerate(pieces):
        a.wait()
        b.wait()
        change = jnp.dot(turned[rows, :], dd[...], preferred_element_type=F32)
        track[rows, :] = (mixed[rows, :] + change * 2048.0 ** -0.5).astype(BF16)
        done.append(pltpu.make_async_copy(track.at[rows], track_out.at[0, rows], out_sem.at[k]))
        done[-1].start()
        if k == PARTS - 2:
            middle.wait()
            done.append(pltpu.make_async_copy(fresh, fresh_out, out_sem.at[PARTS]))
            done[-1].start()
    for copy in done:
        copy.wait()


def on_device(tokens, targets, params, tracker, up_weight, down_weight, edge_weight, step_size):
    hbm = pl.BlockSpec(memory_space=pltpu.HBM)
    smem = pl.BlockSpec(memory_space=pltpu.SMEM)
    block = pltpu.VMEM((2048, 256), BF16)
    out = jax.ShapeDtypeStruct(params.shape, BF16)
    fresh, dd, turned, mixed = pl.pallas_call(
        kernel,
        out_shape=(
            out,
            jax.ShapeDtypeStruct((512, 256), BF16),
            jax.ShapeDtypeStruct((2048, 512), BF16),
            jax.ShapeDtypeStruct((2048, 256), F32),
        ),
        in_specs=[smem, smem] + [hbm] * 6,
        out_specs=(hbm, hbm, hbm, hbm),
        scratch_shapes=[
            pltpu.VMEM((512, 2048), BF16),
            pltpu.VMEM((16, 2048), BF16),
            block, block, block, block, block, block, block,
            pltpu.VMEM((4, 2, 2, 128, 256), BF16),
            pltpu.VMEM((2048, 2048), BF16),
            pltpu.VMEM((512, 256), F32),
            pltpu.VMEM((2, 512, 256), F32),
            pltpu.VMEM((2, 512, 256), BF16),
            pltpu.VMEM((2, 64, 2048), BF16),
            pltpu.VMEM((2, 64, 2048), BF16),
            pltpu.VMEM((2, 16, 2048), BF16),
            pltpu.VMEM((2, 2, 16, 2048), BF16),
            pltpu.VMEM((2, 64, 2048), BF16),
            pltpu.VMEM((2, 512, 256), BF16),
            pltpu.VMEM((2, 512, 256), BF16),
            pltpu.VMEM((512, 256), BF16),
            pltpu.VMEM((1536, 256), BF16),
            pltpu.VMEM((2048, 512), BF16),
            pltpu.VMEM((2048, 256), F32),
            pltpu.SemaphoreType.DMA((SENDS + 4,)),
            pltpu.SemaphoreType.DMA((SEMS,)),
            pltpu.SemaphoreType.DMA((8,)),
        ],
        compiler_params=pltpu.CompilerParams(
            collective_id=0, has_side_effects=True, vmem_limit_bytes=56 * 1024 * 1024
        ),
    )(edge_weight, step_size, tokens, targets, params, tracker, up_weight, down_weight)
    return pl.pallas_call(
        last_kernel,
        out_shape=(out, out),
        in_specs=[hbm] * 4,
        out_specs=(hbm, hbm),
        scratch_shapes=[
            pltpu.VMEM((512, 256), BF16),
            pltpu.VMEM((2048, 512), BF16),
            pltpu.VMEM((2048, 256), F32),
            pltpu.VMEM((1, 2048, 256), BF16),
            block,
            pltpu.SemaphoreType.DMA((2 + 2 * PARTS,)),
            pltpu.SemaphoreType.DMA((1 + PARTS,)),
        ],
    )(dd, turned, mixed, fresh)


def solution(mesh):
    in_specs = (
        P("agent", "tp", None),
        P("agent", "tp", None),
        P("agent", None, "tp"),
        P("agent", None, "tp"),
        P("agent", "tp"),
        P("tp", "agent"),
        P(),
        P(),
    )
    out_specs = (P("agent", None, "tp"), P("agent", None, "tp"))
    return jax.shard_map(
        on_device, mesh=mesh, in_specs=in_specs, out_specs=out_specs, check_vma=False
    )
```
